32 devices in a mesh: section: 1, grp: 16 (over z, x, core), tp: 2 (over y).
Axes of the slice: x: 2, y: 2, z: 4, core: 2. Of those that a mesh axis runs over, the one named last changes fastest.
Arguments:
- partials: bfloat16 [2, 1, 2048, 8192], P('tp', 'section', 'grp'), may hold values from -3 to 3
- residual: bfloat16 [1, 2048, 8192], P('section', 'grp', 'tp'), may hold values from -300 to 300
- norm_gain: bfloat16 [8192], replicated, may hold values from 0.099609375 to 1.8984375
- w_query: bfloat16 [8192, 8192], P('grp', ('section', 'tp')), may hold values from -0.0625 to 0.0625
- w_keyval: bfloat16 [8192, 2048], P('grp', ('section', 'tp')), may hold values from -0.0625 to 0.0625
- bias_query: bfloat16 [8192], P(('section', 'tp')), may hold values from -3 to 3
- bias_keyval: bfloat16 [2048], P(('section', 'tp')), may hold values from -3 to 3
Outputs:
- hidden: bfloat16 [1, 2048, 8192], P('section', 'grp', 'tp')
- query: bfloat16 [1, 2048, 8192], P(None, 'grp', ('section', 'tp'))
- keyval: bfloat16 [1, 2048, 2048], P(None, 'grp', ('section', 'tp'))
The draws below stay inside these ranges and needn't reach their ends.
All inputs are finite; a program needn't handle non-finite values.
Results may differ from the reference program's by a relative error of at most 0.01.
Values may be sent and summed in bfloat16 or wider, within the bound.
A program may use at most 192 MiB of HBM per device.

```python
import jax
import jax.numpy as jnp
from jax import lax

D = 8192
LEN = 2048
SEQS = 1
PARTS_SIZE = 2
QCOLS = 8192
KVCOLS = 2048


def draw_residual(key, part):
    base_key = jax.random.fold_in(key, 11)
    key_normal, key_jitter, key_rows = jax.random.split(base_key, 3)
    column_ramp = 10.0 ** (jnp.arange(D, dtype=jnp.float32) / D)
    column_jitter = jax.random.uniform(key_jitter, (D,), jnp.float32, 0.5, 1.5)
    normal_part = jnp.clip(jax.random.normal(key_normal, (SEQS, LEN, D), jnp.float32), -4.0, 4.0)
    row_scale = 10.0 ** jax.random.uniform(key_rows, (SEQS, LEN, 1), jnp.float32, 0.0, 1.0)
    values = 0.3 * normal_part * column_ramp * column_jitter * row_scale
    return values.astype(jnp.bfloat16)


def block_levels(key, dims, cuts, low, high):
    factor_of = 1.0
    for axis_at, parts in cuts:
        draws = jax.random.uniform(jax.random.fold_in(jax.random.fold_in(key, 6), axis_at), (parts,), jnp.float32, low / len(cuts), high / len(cuts))
        factor_of = factor_of * jnp.repeat(jnp.exp(draws), dims[axis_at] // parts).reshape((-1,) + (1,) * (len(dims) - 1 - axis_at))
    return factor_of


def bell_draw(key, dims, deviation, limit, shards=(), kind=jnp.bfloat16):
    entries = jax.random.normal(key, dims, jnp.float32) * deviation
    if len(shards) > 0:
        entries = block_levels(key, dims, shards, -0.22, 0.18) * entries
    return jnp.clip(entries, min=-limit, max=limit).astype(kind)


def setup_inputs(seed: int = 0) -> dict:
    keys = jax.random.split(jax.random.key(seed), 8)
    partials = bell_draw(keys[0], (PARTS_SIZE, SEQS, LEN, D), 0.5, 3.0, ((0, 2), (2, 16)))
    residual = draw_residual(jax.random.fold_in(keys[7], 71), 0)
    norm_gain = jnp.clip(1.0 + 0.18 * jax.random.normal(keys[2], (D,), jnp.float32), 0.099609375, 1.8984375).astype(jnp.bfloat16)
    w_query = bell_draw(keys[3], (D, QCOLS), D ** -0.5, 0.0625, ((0, 16), (1, 2)))
    w_keyval = bell_draw(keys[4], (D, KVCOLS), D ** -0.5, 0.0625, ((0, 16), (1, 2)))
    bias_query = bell_draw(keys[5], (QCOLS,), 0.5, 3.0, ((0, 2),))
    bias_keyval = bell_draw(keys[6], (KVCOLS,), 0.5, 3.0, ((0, 2),))
    return {"partials": partials, "residual": residual, "norm_gain": norm_gain, "w_query": w_query, "w_keyval": w_keyval, "bias_query": bias_query, "bias_keyval": bias_keyval}


epsilon = 1e-06

def reference(partials, residual, norm_gain, w_query, w_keyval, bias_query, bias_keyval):
    summed = jnp.zeros(residual.shape, jnp.float32)
    for part_index in range(PARTS_SIZE):
        summed = summed + partials[part_index].astype(jnp.float32)
    hidden = (residual.astype(jnp.float32) + summed).astype(jnp.bfloat16)
    widened = hidden.astype(jnp.float32)
    mean_square = lax.optimization_barrier(jnp.mean(widened * widened, axis=-1, keepdims=True))
    normed = (widened * lax.rsqrt(mean_square + epsilon) * norm_gain.astype(jnp.float32)).astype(jnp.bfloat16)
    flattened = normed.reshape(SEQS * LEN, D)
    query = jnp.dot(flattened, w_query, preferred_element_type=jnp.float32) + bias_query.astype(jnp.float32)
    keyval = jnp.dot(flattened, w_keyval, preferred_element_type=jnp.float32) + bias_keyval.astype(jnp.float32)
    query = query.astype(jnp.bfloat16).reshape(SEQS, LEN, QCOLS)
    keyval = keyval.astype(jnp.bfloat16).reshape(SEQS, LEN, KVCOLS)
    return (hidden, query, keyval)
```

```python
import functools
import math

import jax
import jax.numpy as jnp
from jax import lax
from jax.experimental import pallas as pl
from jax.experimental.pallas import tpu as pltpu
from jax.sharding import PartitionSpec as P

epsilon = 1e-06
MESH = pl.DeviceIdType.MESH
CORES = 2
SIDES = 2
LAG = 2


def kernel(ranks, parts, chunks, width, early, fused, *refs):
    refs = list(refs)
    take = lambda n: [refs.pop(0) for _ in range(n)]
    if fused:
        partial_ref, residual_ref, gain_ref = take(3)
    else:
        given_rows, given_squares = take(2)
    wq_ref, wk_ref, bias_ref = take(3)
    if fused:
        hidden_ref, = take(1)
    query_ref, keyval_ref = take(2)
    if fused:
        own_part, own_residual, part_in, rows_ref, square_ref = take(5)
        h_local, p_send, p_recv = take(3)
    else:
        rows_ref, square_ref = given_rows, given_squares
    (xs, wide, products, right_out, right_in, left_out, left_in, squares, scale_ref,
     w_local, m_send, m_recv, wx_send, wx_recv, wf_send, wf_recv,
     x_send, x_recv, f_send, f_recv, q_send, q_recv,
     rt_send, rt_recv, lt_send, lt_recv) = refs

    me = lax.axis_index("grp")
    part = lax.axis_index("tp")
    core = lax.rem(me, CORES)
    chip = me // CORES
    side = lax.rem(chip, SIDES)
    rank = chip // SIDES
    depth, q_cols = wq_ref.shape
    k_cols = wk_ref.shape[1]
    share = SIDES * CORES * depth
    q_steps = q_cols // width
    columns_count = (q_cols + k_cols) // width
    count, feature_share = rows_ref.shape
    rows = count // chunks
    piece = rows // parts
    held = ranks // parts
    steps = chunks * columns_count
    slots = products.shape[0]

    def grp(at_rank, at_side, at_core):
        return (at_rank * SIDES + at_side) * CORES + at_core

    mate = grp(rank, side, 1 - core)
    across = grp(rank, 1 - side, core)

    if fused:
        fills = [
            pltpu.make_async_copy(
                partial_ref.at[:, pl.ds(pl.multiple_of(part * feature_share, feature_share),
                                        feature_share)], own_part, h_local.at[0]),
            pltpu.make_async_copy(residual_ref, own_residual, h_local.at[1])]
        for copy in fills:
            copy.start()

    def w_rows(at_side, at_core):
        return pl.ds(pl.multiple_of((at_side * CORES + at_core) * depth, depth), depth)

    mine = w_rows(side, core)
    locals_ = [pltpu.make_async_copy(wq_ref, wide.at[mine, pl.ds(0, q_cols)], w_local.at[0]),
               pltpu.make_async_copy(wk_ref, wide.at[mine, pl.ds(q_cols, k_cols)], w_local.at[1])]
    for copy in locals_:
        copy.start()

    barrier = pltpu.get_barrier_semaphore()
    for peer in (mate, across):
        pl.semaphore_signal(barrier, inc=1, device_id={"grp": peer}, device_id_type=MESH)
    for d in range(parts):
        for k in range(ranks):
            if d or k:
                pl.semaphore_signal(
                    barrier, inc=1,
                    device_id={"grp": grp(lax.rem(rank + k, ranks), side, core),
                               "tp": lax.rem(part + d, parts)},
                    device_id_type=MESH)
    pl.semaphore_wait(barrier, ranks * parts + 1)

    def p_copy(r, d):
        to = lax.rem(part + d, parts)
        return pltpu.make_async_remote_copy(
            src_ref=partial_ref.at[pl.ds(r * rows, rows),
                                   pl.ds(pl.multiple_of(to * feature_share, feature_share),
                                         feature_share)],
            dst_ref=part_in.at[d - 1, pl.ds(r * rows, rows)],
            send_sem=p_send.at[r, d - 1], recv_sem=p_recv.at[r, d - 1],
            device_id={"tp": to}, device_id_type=MESH)

    if fused:
        for r in range(chunks):
            for d in range(1, parts):
                p_copy(r, d).start()

    def columns(j):
        return pl.ds(pl.multiple_of(j * width, width), width)

    def wx_copy(src, j, to_column):
        return pltpu.make_async_remote_copy(
            src_ref=src.at[:, columns(j)], dst_ref=wide.at[mine, columns(to_column)],
            send_sem=wx_send.at[to_column], recv_sem=wx_recv.at[to_column],
            device_id={"grp": across}, device_id_type=MESH)

    def start_q(j, carry):
        wx_copy(wq_ref, j, j).start()
        return carry

    def start_k(j, carry):
        wx_copy(wk_ref, j, q_steps + j).start()
        return carry

    lax.fori_loop(0, q_steps, start_q, 0)
    lax.fori_loop(0, columns_count - q_steps, start_k, 0)
    m_copies = [pltpu.make_async_remote_copy(
        src_ref=src, dst_ref=dst, send_sem=m_send.at[i], recv_sem=m_recv.at[i],
        device_id={"grp": mate}, device_id_type=MESH)
        for i, (src, dst) in enumerate(((wq_ref, wide.at[mine, pl.ds(0, q_cols)]),
                                        (wk_ref, wide.at[mine, pl.ds(q_cols, k_cols)])))]
    for copy in m_copies:
        copy.start()

    def sum_chunk(r):
        for d in range(1, parts):
            p_copy(r, d).wait_recv()
        here = pl.ds(r * rows, rows)
        block = math.gcd(feature_share, 512)

        def body(c, total):
            at = pl.ds(pl.multiple_of(c * block, block), block)
            value = own_part[here, at].astype(jnp.float32)
            for d in range(1, parts):
                value = value + part_in[d - 1, here, at].astype(jnp.float32)
            value = (own_residual[here, at].astype(jnp.float32) + value).astype(jnp.bfloat16)
            hidden_ref[here, at] = value
            value = value.astype(jnp.float32)
            rows_ref[here, at] = (value * gain_ref[:, at]).astype(jnp.bfloat16)
            value = value * value
            for b in range(block // 128):
                total = total + value[:, b * 128:(b + 1) * 128]
            return total

        total = lax.fori_loop(0, feature_share // block, body, jnp.zeros((rows, 128), jnp.float32))
        square_ref[here, :] = jnp.broadcast_to(
            jnp.sum(total, axis=1, keepdims=True), (rows, 128))

    def piece_at(base, index):
        return pl.ds(pl.multiple_of(base + index * piece, piece), piece)

    def x_ends(r, i, d):
        to = lax.rem(part + d, parts)
        return (rows_ref.at[piece_at(r * rows, to), pl.ds(i * share, share)],
                xs.at[r, piece_at(rank * rows, to)])

    def x_copy(r, i, d):
        src, dst = x_ends(r, i, d)
        return pltpu.make_async_remote_copy(
            src_ref=src, dst_ref=dst, send_sem=x_send.at[r, i, d], recv_sem=x_recv.at[r, rank],
            device_id={"grp": grp(part * held + i, side, core), "tp": lax.rem(part + d, parts)},
            device_id_type=MESH)

    whole_here = rank // held == part

    def x_near(r, i):
        src, dst = x_ends(r, i, 0)
        dst[...] = src[...]

    def each_x(r, far, near):
        for i in range(held):
            here = jnp.logical_and(whole_here, lax.rem(rank, held) == i)
            pl.when(here)(functools.partial(near, r, i))
            pl.when(jnp.logical_not(here))(functools.partial(far, r, i, 0))
            for d in range(1, parts):
                far(r, i, d)

    def x_arrive(r, source):
        at = xs.at[r, piece_at(source * rows, part)]
        pltpu.make_async_remote_copy(
            src_ref=at, dst_ref=at, send_sem=x_send.at[r, 0, 0], recv_sem=x_recv.at[r, source],
            device_id={"grp": mate}, device_id_type=MESH).wait_recv()

    def f_copy(r, source, d):
        at = xs.at[r, piece_at(source * rows, part)]
        return pltpu.make_async_remote_copy(
            src_ref=at, dst_ref=at,
            send_sem=f_send.at[r, source, d - 1], recv_sem=f_recv.at[r, source, d - 1],
            device_id={"tp": lax.rem(part + d, parts)}, device_id_type=MESH)

    def pass_on(r):
        for k in range(ranks):
            source = lax.rem(rank + k, ranks)
            if k:
                x_arrive(r, source)
            else:
                pl.when(jnp.logical_not(whole_here))(functools.partial(x_arrive, r, source))
            for d in range(1, parts):
                f_copy(r, source, d).start()

    def x_wait(r):
        for source in range(ranks):
            for d in range(1, parts):
                at = xs.at[r, piece_at(source * rows, lax.rem(part + parts - d, parts))]
                pltpu.make_async_remote_copy(
                    src_ref=at, dst_ref=at,
                    send_sem=f_send.at[r, source, d - 1], recv_sem=f_recv.at[r, source, d - 1],
                    device_id={"grp": mate}, device_id_type=MESH).wait_recv()

    def q_copy(d):
        return pltpu.make_async_remote_copy(
            src_ref=square_ref, dst_ref=squares.at[d - 1],
            send_sem=q_send.at[d - 1], recv_sem=q_recv.at[d - 1],
            device_id={"tp": lax.rem(part + d, parts)}, device_id_type=MESH)

    if fused:
        for copy in fills:
            copy.wait()
    for r in range(chunks):
        if fused:
            sum_chunk(r)
        each_x(r, lambda r, i, d: x_copy(r, i, d).start(), x_near)
        if r:
            pass_on(r - 1)
    for d in range(1, parts):
        q_copy(d).start()
    pass_on(chunks - 1)

    for copy in locals_:
        copy.wait()
    theirs = w_rows(side, 1 - core)
    for i, (src, dst) in enumerate(((wq_ref, wide.at[theirs, pl.ds(0, q_cols)]),
                                    (wk_ref, wide.at[theirs, pl.ds(q_cols, k_cols)]))):
        pltpu.make_async_remote_copy(
            src_ref=src, dst_ref=dst, send_sem=m_send.at[i], recv_sem=m_recv.at[i],
            device_id={"grp": mate}, device_id_type=MESH).wait_recv()

    mean_square = square_ref[...]
    for d in range(1, parts):
        q_copy(d).wait_recv()
        mean_square = mean_square + squares[d - 1]
    scale_ref[...] = lax.rsqrt(mean_square / (feature_share * parts) + epsilon)

    def wf_copy(j, at_core):
        at = wide.at[w_rows(1 - side, at_core), columns(j)]
        return pltpu.make_async_remote_copy(
            src_ref=at, dst_ref=at, send_sem=wf_send.at[j], recv_sem=wf_recv.at[j],
            device_id={"grp": mate}, device_id_type=MESH)

    def w_arrive(j):
        at = wide.at[w_rows(1 - side, core), columns(j)]
        pltpu.make_async_remote_copy(
            src_ref=at, dst_ref=at, send_sem=wx_send.at[j], recv_sem=wx_recv.at[j],
            device_id={"grp": across}, device_id_type=MESH).wait_recv()
        wf_copy(j, core).start()
        wf_copy(j, 1 - core).wait_recv()

    def place(s):
        first = s < chunks * early
        late = s - chunks * early
        r = jnp.where(first, s // early, lax.rem(late + chunks * early, chunks))
        j = jnp.where(first, lax.rem(s, early), early + late // chunks)
        return r, j

    def multiply(s):
        r, j = place(s)
        pl.when(r == 0)(functools.partial(w_arrive, j))
        for at in range(chunks):
            pl.when(jnp.logical_and(r == at, j == 0))(functools.partial(x_wait, at))
        products[lax.rem(s, slots)] = jnp.dot(
            xs[r], wide[:, columns(j)], preferred_element_type=jnp.float32)

    def chain(out, into, send, recv, s, blocks, to):
        return pltpu.make_async_remote_copy(
            src_ref=out.at[s, pl.ds(0, blocks)], dst_ref=into.at[s, pl.ds(0, blocks)],
            send_sem=send.at[s], recv_sem=recv.at[s],
            device_id={"grp": grp(to, side, core)}, device_id_type=MESH)

    def line(z, going_right, act):
        distance = ranks - 1 - z if going_right else z
        out, into, send, recv = ((right_out, right_in, rt_send, rt_recv) if going_right
                                 else (left_out, left_in, lt_send, lt_recv))
        return functools.partial(act, z, 1 if going_right else -1, distance,
                                 out, into, send, recv)

    def pass_line(z, sign, distance, out, into, send, recv, s):
        ends = ranks - 1 - distance
        slot = lax.rem(s, slots)
        if ends:
            chain(out, into, send, recv, s, distance + 1, z).wait_recv()
        for b in range(distance):
            block = z + sign * (b + 1)
            value = products[slot, pl.ds(block * rows, rows)]
            if ends:
                value = value + into[s, b + 1].astype(jnp.float32)
            out[s, b] = value.astype(jnp.bfloat16)
        if distance:
            chain(out, into, send, recv, s, distance, z + sign).start()

    def drain_line(z, sign, distance, out, into, send, recv, s):
        if distance:
            chain(out, into, send, recv, s, distance, z + sign).wait_send()

    def finish(z, s):
        r, j = place(s)
        slot = lax.rem(s, slots)
        here = pl.ds(pl.multiple_of(r * rows, rows), rows)
        total = products[slot, pl.ds(z * rows, rows)]
        if z:
            total = total + right_in[s, 0].astype(jnp.float32)
        if z < ranks - 1:
            total = total + left_in[s, 0].astype(jnp.float32)
        total = total * scale_ref[here, :][:, :1] + bias_ref[:, columns(j)]
        total = total.astype(jnp.bfloat16)

        def to_query():
            query_ref[here, columns(j)] = total

        def to_keyval():
            keyval_ref[here, columns(j - q_steps)] = total

        pl.when(j < q_steps)(to_query)
        pl.when(j >= q_steps)(to_keyval)

    def step(i, carry):
        pl.when(i < steps)(functools.partial(multiply, i))
        for z in range(ranks):
            def at_rank(z=z):
                for going_right in (True, False):
                    lag = LAG * (z if going_right else ranks - 1 - z)
                    s = i - lag
                    pl.when(jnp.logical_and(s >= 0, s < steps))(
                        functools.partial(line(z, going_right, pass_line), s))
                s = i - LAG * max(z, ranks - 1 - z)
                pl.when(jnp.logical_and(s >= 0, s < steps))(functools.partial(finish, z, s))

            pl.when(rank == z)(at_rank)
        return carry

    lax.fori_loop(0, steps + LAG * (ranks - 1), step, 0)

    if fused:
        for r in range(chunks):
            for d in range(1, parts):
                p_copy(r, d).wait_send()
    for copy in m_copies:
        copy.wait_send()
    for r in range(chunks):
        each_x(r, lambda r, i, d: x_copy(r, i, d).wait_send(), lambda r, i: None)
        for source in range(ranks):
            for d in range(1, parts):
                f_copy(r, source, d).wait_send()
    for d in range(1, parts):
        q_copy(d).wait_send()

    def drain_w(j, carry):
        at = wide.at[mine, columns(j)]
        pltpu.make_async_remote_copy(
            src_ref=at, dst_ref=at, send_sem=wx_send.at[j], recv_sem=wx_recv.at[j],
            device_id={"grp": across}, device_id_type=MESH).wait_send()
        wf_copy(j, core).wait_send()
        return carry

    lax.fori_loop(0, columns_count, drain_w, 0)

    def drain_steps(s, carry):
        for z in range(ranks):
            def at_rank(z=z):
                for going_right in (True, False):
                    line(z, going_right, drain_line)(s)

            pl.when(rank == z)(at_rank)
        return carry

    lax.fori_loop(0, steps, drain_steps, 0)


def project(state, w_query, w_keyval, bias, group, parts, fused):
    if fused:
        count, feature_share = state[1].shape
    else:
        count, feature_share = state[0].shape
    depth, q_cols = w_query.shape
    k_cols = w_keyval.shape[1]
    total = q_cols + k_cols
    width = math.gcd(math.gcd(q_cols, k_cols), 512)
    ranks = group // (CORES * SIDES)
    share = CORES * SIDES * depth
    chunks = min(4, count // (16 * parts))
    rows = count // chunks
    columns_count = total // width
    early = min(3, columns_count)
    steps = chunks * columns_count
    slots = LAG * (ranks - 1) + 1
    held = ranks // parts
    vmem = pl.BlockSpec(memory_space=pltpu.VMEM)
    hbm = pl.BlockSpec(memory_space=pl.ANY)
    dma = pltpu.SemaphoreType.DMA
    bf16 = jnp.bfloat16
    line = pltpu.VMEM((steps, ranks - 1, rows, width), bf16)
    outs = [jax.ShapeDtypeStruct((count, q_cols), bf16),
            jax.ShapeDtypeStruct((count, k_cols), bf16)]
    scratch = []
    if fused:
        outs.insert(0, jax.ShapeDtypeStruct((count, feature_share), bf16))
        scratch = [
            pltpu.VMEM((count, feature_share), bf16),
            pltpu.VMEM((count, feature_share), bf16),
            pltpu.VMEM((parts - 1, count, feature_share), bf16),
            pltpu.VMEM((count, feature_share), bf16),
            pltpu.VMEM((count, 128), jnp.float32),
            dma((2,)), dma((chunks, parts - 1)), dma((chunks, parts - 1)),
        ]
    scratch += [
        pltpu.VMEM((chunks, ranks * rows, share), bf16),
        pltpu.VMEM((share, total), bf16),
        pltpu.VMEM((slots, ranks * rows, width), jnp.float32),
        line, line, line, line,
        pltpu.VMEM((parts - 1, count, 128), jnp.float32),
        pltpu.VMEM((count, 128), jnp.float32),
        dma((2,)), dma((2,)), dma((2,)),
        dma((columns_count,)), dma((columns_count,)),
        dma((columns_count,)), dma((columns_count,)),
        dma((chunks, held, parts)), dma((chunks, ranks)),
        dma((chunks, ranks, parts - 1)), dma((chunks, ranks, parts - 1)),
        dma((parts - 1,)), dma((parts - 1,)),
        dma((steps,)), dma((steps,)), dma((steps,)), dma((steps,)),
    ]
    return pl.pallas_call(
        functools.partial(kernel, ranks, parts, chunks, width, early, fused),
        out_shape=tuple(outs),
        in_specs=([hbm, hbm, vmem] if fused else [vmem, vmem]) + [hbm, hbm, vmem],
        out_specs=(vmem,) * len(outs),
        scratch_shapes=scratch,
        compiler_params=pltpu.CompilerParams(
            collective_id=0, has_side_effects=True, vmem_limit_bytes=62 * 1024 * 1024),
    )(*state, w_query, w_keyval, bias)


def local(group, parts, sections, partials, residual, norm_gain, w_query, w_keyval,
          bias_query, bias_keyval):
    feature_share = residual.shape[2]
    offset = lax.axis_index("tp") * feature_share
    local_gain = lax.dynamic_slice_in_dim(norm_gain, offset, feature_share, 0).astype(jnp.float32)
    bias = jnp.concatenate([bias_query, bias_keyval]).astype(jnp.float32)[None]
    if sections == 1:
        seqs, length = residual.shape[:2]
        count = seqs * length
        hidden, query, keyval = project(
            (partials.reshape(count, -1), residual.reshape(count, -1), local_gain[None]),
            w_query, w_keyval, bias, group, parts, True)
        hidden = hidden.reshape(residual.shape)
    else:
        summed = lax.psum_scatter(
            partials[0], "tp", scatter_dimension=2, tiled=True).astype(jnp.float32)
        hidden = (residual.astype(jnp.float32) + summed).astype(jnp.bfloat16)
        widened = hidden.astype(jnp.float32)
        squares = jnp.sum(widened * widened, axis=-1)
        scaled = (widened * local_gain).astype(jnp.bfloat16)
        scaled = lax.all_gather(scaled, "section", axis=0, tiled=True)
        squares = lax.all_gather(squares, "section", axis=0, tiled=True)
        seqs, length = squares.shape
        count = seqs * length
        squares = jnp.broadcast_to(squares.reshape(-1, 1), (count, 128))
        query, keyval = project(
            (scaled.reshape(count, feature_share), squares), w_query, w_keyval, bias,
            group, parts, False)
    return (hidden, query.reshape(seqs, length, -1), keyval.reshape(seqs, length, -1))


def solution(mesh):
    placed = (
        P("tp", "section", "grp", None),
        P("section", "grp", "tp"),
        P(),
        P("grp", ("section", "tp")),
        P("grp", ("section", "tp")),
        P(("section", "tp")),
        P(("section", "tp")),
    )
    return jax.shard_map(
        functools.partial(local, mesh.shape["grp"], mesh.shape["tp"], mesh.shape["section"]),
        mesh=mesh,
        in_specs=placed,
        out_specs=(
            P("section", "grp", "tp"),
            P(None, "grp", ("section", "tp")),
            P(None, "grp", ("section", "tp")),
        ),
        check_vma=False,
    )
```

```python
import functools
import math

import jax
import jax.numpy as jnp
from jax import lax
from jax.experimental import pallas as pl
from jax.experimental.pallas import tpu as pltpu
from jax.sharding import PartitionSpec as P

epsilon = 1e-06
MESH = pl.DeviceIdType.MESH
CORES = 2
SIDES = 2
LAG = 2
EARLY = 2
EVENTS = (-1.9, 1.5, 2.6, 3.7, 4.75)


def kernel(ranks, parts, chunks, width, early, fused, *refs):
    refs = list(refs)
    take = lambda n: [refs.pop(0) for _ in range(n)]
    if fused:
        partial_ref, residual_ref, gain_ref = take(3)
    else:
        given_rows, given_squares = take(2)
    wq_ref, wk_ref, bias_q_ref, bias_k_ref = take(4)
    if fused:
        hidden_ref, = take(1)
    query_ref, keyval_ref = take(2)
    if fused:
        own_part, own_residual, part_in, rows_ref, square_ref = take(5)
        gain_row, h_local, p_send, p_recv = take(4)
    else:
        rows_ref, square_ref = given_rows, given_squares
    (bias_row, others, xs, wide, products, right_out, right_in, left_out, left_in, squares, scale_ref,
     w_local, m_send, m_recv, wx_send, wx_recv, wf_send, wf_recv,
     y_send, y_recv, x_send, x_recv, f_send, f_recv, q_send, q_recv,
     rt_send, rt_recv, lt_send, lt_recv) = refs

    me = lax.axis_index("grp")
    part = lax.axis_index("tp")
    core = lax.rem(me, CORES)
    chip = me // CORES
    side = lax.rem(chip, SIDES)
    rank = chip // SIDES
    depth, q_cols = wq_ref.shape
    k_cols = wk_ref.shape[1]
    share = SIDES * CORES * depth
    q_steps = q_cols // width
    columns_count = (q_cols + k_cols) // width
    count, feature_share = rows_ref.shape
    rows = count // chunks
    piece = rows // parts
    held = ranks // parts
    steps = chunks * columns_count
    slots = products.shape[0]

    def grp(at_rank, at_side, at_core):
        return (at_rank * SIDES + at_side) * CORES + at_core

    mate = grp(rank, side, 1 - core)
    across = grp(rank, 1 - side, core)

    if fused:
        fills = [
            pltpu.make_async_copy(
                partial_ref.at[:, pl.ds(pl.multiple_of(part * feature_share, feature_share),
                                        feature_share)], own_part, h_local.at[0]),
            pltpu.make_async_copy(residual_ref, own_residual, h_local.at[1])]
        for copy in fills:
            copy.start()

    def w_rows(at_side, at_core):
        return pl.ds(pl.multiple_of((at_side * CORES + at_core) * depth, depth), depth)

    mine = w_rows(side, core)
    locals_ = [pltpu.make_async_copy(wq_ref, wide.at[mine, pl.ds(0, q_cols)], w_local.at[0]),
               pltpu.make_async_copy(wk_ref, wide.at[mine, pl.ds(q_cols, k_cols)], w_local.at[1])]
    for copy in locals_:
        copy.start()

    barrier = pltpu.get_barrier_semaphore()
    for peer in (mate, across):
        pl.semaphore_signal(barrier, inc=1, device_id={"grp": peer}, device_id_type=MESH)
    for k in range(1, ranks):
        pl.semaphore_signal(
            barrier, inc=1, device_id={"grp": grp(lax.rem(rank + k, ranks), side, core)},
            device_id_type=MESH)
    for d in range(1, parts):
        pl.semaphore_signal(
            barrier, inc=1, device_id={"tp": lax.rem(part + d, parts)}, device_id_type=MESH)
    pl.semaphore_wait(barrier, ranks + parts)

    def spread(src, start, length, dst, to):
        block = math.gcd(length, 1024)
        for b in range(length // block):
            value = src[pl.ds(start + b * block, block)].astype(jnp.float32)
            dst[:, pl.ds(to + b * block, block)] = value.reshape(1, block)

    def p_copy(r, d):
        to = lax.rem(part + d, parts)
        return pltpu.make_async_remote_copy(
            src_ref=partial_ref.at[pl.ds(r * rows, rows),
                                   pl.ds(pl.multiple_of(to * feature_share, feature_share),
                                         feature_share)],
            dst_ref=part_in.at[d - 1, pl.ds(r * rows, rows)],
            send_sem=p_send.at[r, d - 1], recv_sem=p_recv.at[r, d - 1],
            device_id={"tp": to}, device_id_type=MESH)

    def send_part(r):
        for d in range(1, parts):
            p_copy(r, d).start()

    if fused:
        for r in range(min(2, chunks)):
            send_part(r)
        spread(gain_ref, pl.multiple_of(part * feature_share, feature_share), feature_share,
               gain_row, 0)
    spread(bias_q_ref, 0, q_cols, bias_row, 0)
    spread(bias_k_ref, 0, k_cols, bias_row, q_cols)

    def columns(j):
        return pl.ds(pl.multiple_of(j * width, width), width)

    def wx_copy(src, j, to_column):
        return pltpu.make_async_remote_copy(
            src_ref=src.at[:, columns(j)], dst_ref=wide.at[mine, columns(to_column)],
            send_sem=wx_send.at[to_column], recv_sem=wx_recv.at[to_column],
            device_id={"grp": across}, device_id_type=MESH)

    def start_q(j, carry):
        wx_copy(wq_ref, j, j).start()
        return carry

    def start_k(j, carry):
        wx_copy(wk_ref, j, q_steps + j).start()
        return carry

    lax.fori_loop(0, q_steps, start_q, 0)
    lax.fori_loop(0, columns_count - q_steps, start_k, 0)
    m_copies = [pltpu.make_async_remote_copy(
        src_ref=src, dst_ref=dst, send_sem=m_send.at[i], recv_sem=m_recv.at[i],
        device_id={"grp": mate}, device_id_type=MESH)
        for i, (src, dst) in enumerate(((wq_ref, wide.at[mine, pl.ds(0, q_cols)]),
                                        (wk_ref, wide.at[mine, pl.ds(q_cols, k_cols)])))]
    for copy in m_copies:
        copy.start()

    def sum_chunk(r):
        for d in range(1, parts):
            p_copy(r, d).wait_recv()
        here = pl.ds(r * rows, rows)
        block = math.gcd(feature_share, 512)

        def body(c, total):
            at = pl.ds(pl.multiple_of(c * block, block), block)
            value = own_part[here, at].astype(jnp.float32)
            for d in range(1, parts):
                value = value + part_in[d - 1, here, at].astype(jnp.float32)
            value = (own_residual[here, at].astype(jnp.float32) + value).astype(jnp.bfloat16)
            hidden_ref[here, at] = value
            value = value.astype(jnp.float32)
            rows_ref[here, at] = (value * gain_row[:, at]).astype(jnp.bfloat16)
            value = value * value
            for b in range(block // 128):
                total = total + value[:, b * 128:(b + 1) * 128]
            return total

        total = lax.fori_loop(0, feature_share // block, body, jnp.zeros((rows, 128), jnp.float32))
        square_ref[here, :] = jnp.broadcast_to(
            jnp.sum(total, axis=1, keepdims=True), (rows, 128))

    def piece_at(base, index):
        return pl.ds(pl.multiple_of(base + index * piece, piece), piece)

    def y_copy(r, d):
        to = lax.rem(part + d, parts)
        return pltpu.make_async_remote_copy(
            src_ref=rows_ref.at[piece_at(r * rows, to)],
            dst_ref=others.at[d - 1, pl.ds(r * piece, piece)],
            send_sem=y_send.at[r, d - 1], recv_sem=y_recv.at[r, d - 1],
            device_id={"tp": to}, device_id_type=MESH)

    def x_ends(r, d, i):
        features = pl.ds(i * share, share)
        src = (others.at[d - 1, pl.ds(r * piece, piece), features] if d
               else rows_ref.at[piece_at(r * rows, part), features])
        return src, xs.at[r, piece_at(rank * rows, part)]

    def x_to(d, i):
        return lax.rem(part + parts - d, parts) * held + i

    def x_copy(r, d, i):
        src, dst = x_ends(r, d, i)
        return pltpu.make_async_remote_copy(
            src_ref=src, dst_ref=dst, send_sem=x_send.at[r, d, i], recv_sem=x_recv.at[r, rank],
            device_id={"grp": grp(x_to(d, i), side, core)}, device_id_type=MESH)

    def each_x(r, d, far, near):
        for i in range(held):
            here = x_to(d, i) == rank
            if near is not None:
                pl.when(here)(functools.partial(near, r, d, i))
            pl.when(jnp.logical_not(here))(functools.partial(far, r, d, i))

    def x_near(r, d, i):
        src, dst = x_ends(r, d, i)
        dst[...] = src[...]

    def x_start(r, d):
        each_x(r, d, lambda r, d, i: x_copy(r, d, i).start(), x_near)

    def relay(r):
        for d in range(1, parts):
            y_copy(r, d).wait_recv()
            x_start(r, d)

    def f_copy(r, source, d):
        at = xs.at[r, piece_at(source * rows, part)]
        return pltpu.make_async_remote_copy(
            src_ref=at, dst_ref=at,
            send_sem=f_send.at[r, source, d - 1], recv_sem=f_recv.at[r, source, d - 1],
            device_id={"tp": lax.rem(part + d, parts)}, device_id_type=MESH)

    def pass_on(r):
        for k in range(ranks):
            source = lax.rem(rank + k, ranks)
            if k:
                at = xs.at[r, piece_at(source * rows, part)]
                pltpu.make_async_remote_copy(
                    src_ref=at, dst_ref=at, send_sem=x_send.at[r, 0, 0],
                    recv_sem=x_recv.at[r, source],
                    device_id={"grp": mate}, device_id_type=MESH).wait_recv()
            for d in range(1, parts):
                f_copy(r, source, d).start()

    def x_wait(r):
        for source in range(ranks):
            for d in range(1, parts):
                at = xs.at[r, piece_at(source * rows, lax.rem(part + parts - d, parts))]
                pltpu.make_async_remote_copy(
                    src_ref=at, dst_ref=at,
                    send_sem=f_send.at[r, source, d - 1], recv_sem=f_recv.at[r, source, d - 1],
                    device_id={"grp": mate}, device_id_type=MESH).wait_recv()

    def q_copy(r, d):
        here = pl.ds(r * rows, rows)
        return pltpu.make_async_remote_copy(
            src_ref=square_ref.at[here], dst_ref=squares.at[d - 1, here],
            send_sem=q_send.at[r, d - 1], recv_sem=q_recv.at[r, d - 1],
            device_id={"tp": lax.rem(part + d, parts)}, device_id_type=MESH)

    def prepare(r):
        if fused:
            sum_chunk(r)
        for d in range(1, parts):
            y_copy(r, d).start()
        x_start(r, 0)
        for d in range(1, parts):
            q_copy(r, d).start()

    if fused:
        for copy in fills:
            copy.wait()

    def set_scale(r):
        here = pl.ds(r * rows, rows)
        mean_square = square_ref[here]
        for d in range(1, parts):
            q_copy(r, d).wait_recv()
            mean_square = mean_square + squares[d - 1, here]
        scale_ref[here] = lax.rsqrt(mean_square / (feature_share * parts) + epsilon)

    def wf_copy(j, at_core):
        at = wide.at[w_rows(1 - side, at_core), columns(j)]
        return pltpu.make_async_remote_copy(
            src_ref=at, dst_ref=at, send_sem=wf_send.at[j], recv_sem=wf_recv.at[j],
            device_id={"grp": mate}, device_id_type=MESH)

    def w_arrive(j):
        at = wide.at[w_rows(1 - side, core), columns(j)]
        pltpu.make_async_remote_copy(
            src_ref=at, dst_ref=at, send_sem=wx_send.at[j], recv_sem=wx_recv.at[j],
            device_id={"grp": across}, device_id_type=MESH).wait_recv()
        wf_copy(j, core).start()
        wf_copy(j, 1 - core).wait_recv()

    runs = []
    for r in range(chunks):
        before = min(columns_count, early + min(r - 1, 1)) if r else 0
        after = columns_count if r == chunks - 1 else min(columns_count, early + min(r, 1))
        if before:
            runs.append((r, 1, 0, before))
        if after > before:
            runs.append((0, r + 1, before, after))
    ends = [0]
    segments = [0] * chunks
    for r0, nr, j0, j1 in runs:
        ends.append(ends[-1] + nr * (j1 - j0))
        segments[r0 + nr - 1] = ends[-1]

    def place(s):
        r, j = s, s
        for (r0, nr, j0, _), begin in zip(runs, ends):
            inside = s >= begin
            r = jnp.where(inside, r0 + lax.rem(s - begin, nr), r)
            j = jnp.where(inside, j0 + (s - begin) // nr, j)
        return r, j

    def multiply(s):
        r, j = place(s)
        pl.when(r == 0)(functools.partial(w_arrive, j))
        products[lax.rem(s, slots)] = jnp.dot(
            xs[r], wide[:, columns(j)], preferred_element_type=jnp.float32)

    def chain(out, into, send, recv, s, blocks, to):
        return pltpu.make_async_remote_copy(
            src_ref=out.at[s, pl.ds(0, blocks)], dst_ref=into.at[s, pl.ds(0, blocks)],
            send_sem=send.at[s], recv_sem=recv.at[s],
            device_id={"grp": grp(to, side, core)}, device_id_type=MESH)

    def line(z, going_right, act):
        distance = ranks - 1 - z if going_right else z
        out, into, send, recv = ((right_out, right_in, rt_send, rt_recv) if going_right
                                 else (left_out, left_in, lt_send, lt_recv))
        return functools.partial(act, z, 1 if going_right else -1, distance,
                                 out, into, send, recv)

    def pass_line(z, sign, distance, out, into, send, recv, s):
        ends = ranks - 1 - distance
        slot = lax.rem(s, slots)
        if ends:
            chain(out, into, send, recv, s, distance + 1, z).wait_recv()
        for b in range(distance):
            block = z + sign * (b + 1)
            value = products[slot, pl.ds(block * rows, rows)]
            if ends:
                value = value + into[s, b + 1].astype(jnp.float32)
            out[s, b] = value.astype(jnp.bfloat16)
        if distance:
            chain(out, into, send, recv, s, distance, z + sign).start()

    def drain_line(z, sign, distance, out, into, send, recv, s):
        if distance:
            chain(out, into, send, recv, s, distance, z + sign).wait_send()

    def finish(z, s):
        r, j = place(s)
        slot = lax.rem(s, slots)
        here = pl.ds(pl.multiple_of(r * rows, rows), rows)
        total = products[slot, pl.ds(z * rows, rows)]
        if z:
            total = total + right_in[s, 0].astype(jnp.float32)
        if z < ranks - 1:
            total = total + left_in[s, 0].astype(jnp.float32)
        total = total * scale_ref[here, :][:, :1] + bias_row[:, columns(j)]
        total = total.astype(jnp.bfloat16)

        def to_query():
            query_ref[here, columns(j)] = total

        def to_keyval():
            keyval_ref[here, columns(j - q_steps)] = total

        pl.when(j < q_steps)(to_query)
        pl.when(j >= q_steps)(to_keyval)

    def step(i, carry):
        pl.when(i < steps)(functools.partial(multiply, i))
        for z in range(ranks):
            def at_rank(z=z):
                for going_right in (True, False):
                    lag = LAG * (z if going_right else ranks - 1 - z)
                    s = i - lag
                    pl.when(jnp.logical_and(s >= 0, s < steps))(
                        functools.partial(line(z, going_right, pass_line), s))
                s = i - LAG * max(z, ranks - 1 - z)
                pl.when(jnp.logical_and(s >= 0, s < steps))(functools.partial(finish, z, s))

            pl.when(rank == z)(at_rank)
        return carry

    def load_own():
        for copy in locals_:
            copy.wait()
        theirs = w_rows(side, 1 - core)
        for i, (src, dst) in enumerate(((wq_ref, wide.at[theirs, pl.ds(0, q_cols)]),
                                        (wk_ref, wide.at[theirs, pl.ds(q_cols, k_cols)]))):
            pltpu.make_async_remote_copy(
                src_ref=src, dst_ref=dst, send_sem=m_send.at[i], recv_sem=m_recv.at[i],
                device_id={"grp": mate}, device_id_type=MESH).wait_recv()

    def segment(r):
        if r == 0:
            load_own()
        x_wait(r)
        set_scale(r)
        lax.fori_loop(segments[r - 1] if r else 0,
                      segments[r] + (LAG * (ranks - 1) if r == chunks - 1 else 0), step, 0)

    at = EVENTS
    events = []
    for r in range(chunks):
        events += [(r, prepare, r), (r + at[1], relay, r), (r + at[2], pass_on, r),
                   (r + (at[4] if r else at[3]), segment, r)]
        if fused and r > 1:
            events.append((r + at[0], send_part, r))
    for _, event, r in sorted(events, key=lambda e: e[0]):
        event(r)

    if fused:
        for r in range(chunks):
            for d in range(1, parts):
                p_copy(r, d).wait_send()
    for copy in m_copies:
        copy.wait_send()
    for r in range(chunks):
        for d in range(parts):
            each_x(r, d, lambda r, d, i: x_copy(r, d, i).wait_send(), None)
        for d in range(1, parts):
            y_copy(r, d).wait_send()
            for source in range(ranks):
                f_copy(r, source, d).wait_send()
        for d in range(1, parts):
            q_copy(r, d).wait_send()

    def drain_w(j, carry):
        at = wide.at[mine, columns(j)]
        pltpu.make_async_remote_copy(
            src_ref=at, dst_ref=at, send_sem=wx_send.at[j], recv_sem=wx_recv.at[j],
            device_id={"grp": across}, device_id_type=MESH).wait_send()
        wf_copy(j, core).wait_send()
        return carry

    lax.fori_loop(0, columns_count, drain_w, 0)

    def drain_steps(s, carry):
        for z in range(ranks):
            def at_rank(z=z):
                for going_right in (True, False):
                    line(z, going_right, drain_line)(s)

            pl.when(rank == z)(at_rank)
        return carry

    lax.fori_loop(0, steps, drain_steps, 0)


def project(state, w_query, w_keyval, biases, group, parts, fused):
    if fused:
        count, feature_share = state[1].shape
    else:
        count, feature_share = state[0].shape
    depth, q_cols = w_query.shape
    k_cols = w_keyval.shape[1]
    total = q_cols + k_cols
    width = math.gcd(math.gcd(q_cols, k_cols), 512)
    ranks = group // (CORES * SIDES)
    share = CORES * SIDES * depth
    chunks = min(4, count // (16 * parts))
    rows = count // chunks
    columns_count = total // width
    early = min(EARLY, columns_count)
    steps = chunks * columns_count
    slots = LAG * (ranks - 1) + 1
    held = ranks // parts
    vmem = pl.BlockSpec(memory_space=pltpu.VMEM)
    hbm = pl.BlockSpec(memory_space=pl.ANY)
    dma = pltpu.SemaphoreType.DMA
    bf16 = jnp.bfloat16
    line = pltpu.VMEM((steps, ranks - 1, rows, width), bf16)
    outs = [jax.ShapeDtypeStruct((count, q_cols), bf16),
            jax.ShapeDtypeStruct((count, k_cols), bf16)]
    scratch = []
    if fused:
        outs.insert(0, jax.ShapeDtypeStruct((count, feature_share), bf16))
        scratch = [
            pltpu.VMEM((count, feature_share), bf16),
            pltpu.VMEM((count, feature_share), bf16),
            pltpu.VMEM((parts - 1, count, feature_share), bf16),
            pltpu.VMEM((count, feature_share), bf16),
            pltpu.VMEM((count, 128), jnp.float32),
            pltpu.VMEM((1, feature_share), jnp.float32),
            dma((2,)), dma((chunks, parts - 1)), dma((chunks, parts - 1)),
        ]
    scratch += [
        pltpu.VMEM((1, total), jnp.float32),
        pltpu.VMEM((parts - 1, count // parts, feature_share), bf16),
        pltpu.VMEM((chunks, ranks * rows, share), bf16),
        pltpu.VMEM((share, total), bf16),
        pltpu.VMEM((slots, ranks * rows, width), jnp.float32),
        line, line, line, line,
        pltpu.VMEM((parts - 1, count, 128), jnp.float32),
        pltpu.VMEM((count, 128), jnp.float32),
        dma((2,)), dma((2,)), dma((2,)),
        dma((columns_count,)), dma((columns_count,)),
        dma((columns_count,)), dma((columns_count,)),
        dma((chunks, parts - 1)), dma((chunks, parts - 1)),
        dma((chunks, parts, held)), dma((chunks, ranks)),
        dma((chunks, ranks, parts - 1)), dma((chunks, ranks, parts - 1)),
        dma((chunks, parts - 1)), dma((chunks, parts - 1)),
        dma((steps,)), dma((steps,)), dma((steps,)), dma((steps,)),
    ]
    return pl.pallas_call(
        functools.partial(kernel, ranks, parts, chunks, width, early, fused),
        out_shape=tuple(outs),
        in_specs=([hbm, hbm, vmem] if fused else [vmem, vmem]) + [hbm, hbm, vmem, vmem],
        out_specs=(vmem,) * len(outs),
        scratch_shapes=scratch,
        compiler_params=pltpu.CompilerParams(
            collective_id=0, has_side_effects=True, vmem_limit_bytes=62 * 1024 * 1024),
    )(*state, w_query, w_keyval, *biases)


def hand_over(cuts, *refs):
    count = len(cuts)
    sources, targets = refs[:count], refs[count:2 * count]
    buffers, taken, given = refs[2 * count:3 * count], refs[-2], refs[-1]

    def copies(i, c):
        rows = sources[i].shape[0] // cuts[i]
        here = pl.ds(c * rows, rows)
        return (pltpu.make_async_copy(sources[i].at[here], buffers[i].at[here], taken.at[i, c]),
                pltpu.make_async_copy(buffers[i].at[here], targets[i].at[here], given.at[i, c]))

    every = [copies(i, c) for i in range(count) for c in range(cuts[i])]
    for copy, _ in every:
        copy.start()
    for copy, onward in every:
        copy.wait()
        onward.start()
    for _, onward in every:
        onward.wait()


def place(*arrays):
    cuts = [4 if a.shape[0] * a.shape[1] > 2 ** 18 and a.shape[0] % 64 == 0 else 1 for a in arrays]
    anywhere = pl.BlockSpec(memory_space=pl.ANY)
    dma = pltpu.SemaphoreType.DMA
    return pl.pallas_call(
        functools.partial(hand_over, cuts),
        out_shape=tuple(jax.ShapeDtypeStruct(a.shape, a.dtype) for a in arrays),
        in_specs=[anywhere] * len(arrays),
        out_specs=(anywhere,) * len(arrays),
        scratch_shapes=[pltpu.VMEM(a.shape, a.dtype) for a in arrays] + [
            dma((len(arrays), max(cuts))), dma((len(arrays), max(cuts)))],
    )(*arrays)


def local(group, parts, sections, partials, residual, norm_gain, w_query, w_keyval,
          bias_query, bias_keyval):
    feature_share = residual.shape[2]
    biases = (bias_query, bias_keyval)
    if sections == 1:
        seqs, length = residual.shape[:2]
        count = seqs * length
        hidden, query, keyval = project(
            (partials.reshape(count, -1), residual.reshape(count, -1), norm_gain),
            w_query, w_keyval, biases, group, parts, True)
        hidden, query, keyval = place(hidden, query, keyval)
        hidden = hidden.reshape(residual.shape)
    else:
        offset = lax.axis_index("tp") * feature_share
        local_gain = lax.dynamic_slice_in_dim(
            norm_gain, offset, feature_share, 0).astype(jnp.float32)
        summed = lax.psum_scatter(
            partials[0], "tp", scatter_dimension=2, tiled=True).astype(jnp.float32)
        hidden = (residual.astype(jnp.float32) + summed).astype(jnp.bfloat16)
        widened = hidden.astype(jnp.float32)
        squares = jnp.sum(widened * widened, axis=-1)
        scaled = (widened * local_gain).astype(jnp.bfloat16)
        scaled = lax.all_gather(scaled, "section", axis=0, tiled=True)
        squares = lax.all_gather(squares, "section", axis=0, tiled=True)
        seqs, length = squares.shape
        count = seqs * length
        squares = jnp.broadcast_to(squares.reshape(-1, 1), (count, 128))
        query, keyval = project(
            (scaled.reshape(count, feature_share), squares), w_query, w_keyval, biases,
            group, parts, False)
    return (hidden, query.reshape(seqs, length, -1), keyval.reshape(seqs, length, -1))


def solution(mesh):
    placed = (
        P("tp", "section", "grp", None),
        P("section", "grp", "tp"),
        P(),
        P("grp", ("section", "tp")),
        P("grp", ("section", "tp")),
        P(("section", "tp")),
        P(("section", "tp")),
    )
    return jax.shard_map(
        functools.partial(local, mesh.shape["grp"], mesh.shape["tp"], mesh.shape["section"]),
        mesh=mesh,
        in_specs=placed,
        out_specs=(
            P("section", "grp", "tp"),
            P(None, "grp", ("section", "tp")),
            P(None, "grp", ("section", "tp")),
        ),
        check_vma=False,
    )
```

```python
import functools
import math

import jax
import jax.numpy as jnp
from jax import lax
from jax.experimental import pallas as pl
from jax.experimental.pallas import tpu as pltpu
from jax.sharding import PartitionSpec as P

epsilon = 1e-06
MESH = pl.DeviceIdType.MESH
CORES = 2
SIDES = 2
LAG = 2
EARLY = 2


def kernel(ranks, parts, chunks, width, early, fused, *refs):
    refs = list(refs)
    take = lambda n: [refs.pop(0) for _ in range(n)]
    if fused:
        partial_ref, residual_ref, gain_ref = take(3)
    else:
        given_rows, given_squares = take(2)
    wq_ref, wk_ref, bias_q_ref, bias_k_ref = take(4)
    if fused:
        hidden_ref, = take(1)
    query_ref, keyval_ref = take(2)
    if fused:
        own_part, own_residual, part_in, rows_ref, square_ref = take(5)
        gain_row, h_local, p_send, p_recv = take(4)
    else:
        rows_ref, square_ref = given_rows, given_squares
    (bias_row, others, xs, wide, products, right_out, right_in, left_out, left_in, squares, scale_ref,
     w_local, m_send, m_recv, wx_send, wx_recv, wf_send, wf_recv,
     y_send, y_recv, x_send, x_recv, f_send, f_recv, q_send, q_recv,
     rt_send, rt_recv, lt_send, lt_recv) = refs

    me = lax.axis_index("grp")
    part = lax.axis_index("tp")
    core = lax.rem(me, CORES)
    chip = me // CORES
    side = lax.rem(chip, SIDES)
    rank = chip // SIDES
    depth, q_cols = wq_ref.shape
    k_cols = wk_ref.shape[1]
    share = SIDES * CORES * depth
    q_steps = q_cols // width
    columns_count = (q_cols + k_cols) // width
    count, feature_share = rows_ref.shape
    rows = count // chunks
    piece = rows // parts
    held = ranks // parts
    steps = chunks * columns_count
    slots = products.shape[0]

    def grp(at_rank, at_side, at_core):
        return (at_rank * SIDES + at_side) * CORES + at_core

    mate = grp(rank, side, 1 - core)
    across = grp(rank, 1 - side, core)

    if fused:
        fills = [
            pltpu.make_async_copy(
                partial_ref.at[:, pl.ds(pl.multiple_of(part * feature_share, feature_share),
                                        feature_share)], own_part, h_local.at[0]),
            pltpu.make_async_copy(residual_ref, own_residual, h_local.at[1])]
        for copy in fills:
            copy.start()

    def w_rows(at_side, at_core):
        return pl.ds(pl.multiple_of((at_side * CORES + at_core) * depth, depth), depth)

    mine = w_rows(side, core)
    locals_ = [pltpu.make_async_copy(wq_ref, wide.at[mine, pl.ds(0, q_cols)], w_local.at[0]),
               pltpu.make_async_copy(wk_ref, wide.at[mine, pl.ds(q_cols, k_cols)], w_local.at[1])]
    for copy in locals_:
        copy.start()

    barrier = pltpu.get_barrier_semaphore()
    for peer in (mate, across):
        pl.semaphore_signal(barrier, inc=1, device_id={"grp": peer}, device_id_type=MESH)
    for k in range(1, ranks):
        pl.semaphore_signal(
            barrier, inc=1, device_id={"grp": grp(lax.rem(rank + k, ranks), side, core)},
            device_id_type=MESH)
    for d in range(1, parts):
        pl.semaphore_signal(
            barrier, inc=1, device_id={"tp": lax.rem(part + d, parts)}, device_id_type=MESH)
    pl.semaphore_wait(barrier, ranks + parts)

    def spread(src, start, length, dst, to):
        block = math.gcd(length, 1024)
        for b in range(length // block):
            value = src[pl.ds(start + b * block, block)].astype(jnp.float32)
            dst[:, pl.ds(to + b * block, block)] = value.reshape(1, block)

    def p_copy(r, d):
        to = lax.rem(part + d, parts)
        return pltpu.make_async_remote_copy(
            src_ref=partial_ref.at[pl.ds(r * rows, rows),
                                   pl.ds(pl.multiple_of(to * feature_share, feature_share),
                                         feature_share)],
            dst_ref=part_in.at[d - 1, pl.ds(r * rows, rows)],
            send_sem=p_send.at[r, d - 1], recv_sem=p_recv.at[r, d - 1],
            device_id={"tp": to}, device_id_type=MESH)

    def send_part(r):
        for d in range(1, parts):
            p_copy(r, d).start()

    if fused:
        for r in range(min(2, chunks)):
            send_part(r)
        spread(gain_ref, pl.multiple_of(part * feature_share, feature_share), feature_share,
               gain_row, 0)
    spread(bias_q_ref, 0, q_cols, bias_row, 0)
    spread(bias_k_ref, 0, k_cols, bias_row, q_cols)

    def columns(j):
        return pl.ds(pl.multiple_of(j * width, width), width)

    def wx_copy(src, j, to_column):
        return pltpu.make_async_remote_copy(
            src_ref=src.at[:, columns(j)], dst_ref=wide.at[mine, columns(to_column)],
            send_sem=wx_send.at[to_column], recv_sem=wx_recv.at[to_column],
            device_id={"grp": across}, device_id_type=MESH)

    def start_q(j, carry):
        wx_copy(wq_ref, j, j).start()
        return carry

    def start_k(j, carry):
        wx_copy(wk_ref, j, q_steps + j).start()
        return carry

    lax.fori_loop(0, q_steps, start_q, 0)
    lax.fori_loop(0, columns_count - q_steps, start_k, 0)
    m_copies = [pltpu.make_async_remote_copy(
        src_ref=src, dst_ref=dst, send_sem=m_send.at[i], recv_sem=m_recv.at[i],
        device_id={"grp": mate}, device_id_type=MESH)
        for i, (src, dst) in enumerate(((wq_ref, wide.at[mine, pl.ds(0, q_cols)]),
                                        (wk_ref, wide.at[mine, pl.ds(q_cols, k_cols)])))]
    for copy in m_copies:
        copy.start()

    def sum_chunk(r):
        for d in range(1, parts):
            p_copy(r, d).wait_recv()
        here = pl.ds(r * rows, rows)
        block = math.gcd(feature_share, 512)

        def body(c, total):
            at = pl.ds(pl.multiple_of(c * block, block), block)
            value = own_part[here, at].astype(jnp.float32)
            for d in range(1, parts):
                value = value + part_in[d - 1, here, at].astype(jnp.float32)
            value = (own_residual[here, at].astype(jnp.float32) + value).astype(jnp.bfloat16)
            hidden_ref[here, at] = value
            value = value.astype(jnp.float32)
            rows_ref[here, at] = (value * gain_row[:, at]).astype(jnp.bfloat16)
            value = value * value
            for b in range(block // 128):
                total = total + value[:, b * 128:(b + 1) * 128]
            return total

        total = lax.fori_loop(0, feature_share // block, body, jnp.zeros((rows, 128), jnp.float32))
        square_ref[here, :] = jnp.broadcast_to(
            jnp.sum(total, axis=1, keepdims=True), (rows, 128))

    def piece_at(base, index):
        return pl.ds(pl.multiple_of(base + index * piece, piece), piece)

    def y_copy(r, d):
        to = lax.rem(part + d, parts)
        return pltpu.make_async_remote_copy(
            src_ref=rows_ref.at[piece_at(r * rows, to)],
            dst_ref=others.at[d - 1, pl.ds(r * piece, piece)],
            send_sem=y_send.at[r, d - 1], recv_sem=y_recv.at[r, d - 1],
            device_id={"tp": to}, device_id_type=MESH)

    def x_ends(r, d, i):
        features = pl.ds(i * share, share)
        src = (others.at[d - 1, pl.ds(r * piece, piece), features] if d
               else rows_ref.at[piece_at(r * rows, part), features])
        return src, xs.at[r, piece_at(rank * rows, part)]

    def x_to(d, i):
        return lax.rem(part + parts - d, parts) * held + i

    def x_copy(r, d, i):
        src, dst = x_ends(r, d, i)
        return pltpu.make_async_remote_copy(
            src_ref=src, dst_ref=dst, send_sem=x_send.at[r, d, i], recv_sem=x_recv.at[r, rank],
            device_id={"grp": grp(x_to(d, i), side, core)}, device_id_type=MESH)

    def each_x(r, d, far, near):
        for i in range(held):
            here = x_to(d, i) == rank
            if near is not None:
                pl.when(here)(functools.partial(near, r, d, i))
            pl.when(jnp.logical_not(here))(functools.partial(far, r, d, i))

    def x_near(r, d, i):
        src, dst = x_ends(r, d, i)
        dst[...] = src[...]

    def x_start(r, d):
        each_x(r, d, lambda r, d, i: x_copy(r, d, i).start(), x_near)

    def relay(r):
        for d in range(1, parts):
            y_copy(r, d).wait_recv()
            x_start(r, d)

    def f_copy(r, source, d):
        at = xs.at[r, piece_at(source * rows, part)]
        return pltpu.make_async_remote_copy(
            src_ref=at, dst_ref=at,
            send_sem=f_send.at[r, source, d - 1], recv_sem=f_recv.at[r, source, d - 1],
            device_id={"tp": lax.rem(part + d, parts)}, device_id_type=MESH)

    def pass_on(r):
        for k in range(ranks):
            source = lax.rem(rank + k, ranks)
            if k:
                at = xs.at[r, piece_at(source * rows, part)]
                pltpu.make_async_remote_copy(
                    src_ref=at, dst_ref=at, send_sem=x_send.at[r, 0, 0],
                    recv_sem=x_recv.at[r, source],
                    device_id={"grp": mate}, device_id_type=MESH).wait_recv()
            for d in range(1, parts):
                f_copy(r, source, d).start()

    def x_wait(r):
        for source in range(ranks):
            for d in range(1, parts):
                at = xs.at[r, piece_at(source * rows, lax.rem(part + parts - d, parts))]
                pltpu.make_async_remote_copy(
                    src_ref=at, dst_ref=at,
                    send_sem=f_send.at[r, source, d - 1], recv_sem=f_recv.at[r, source, d - 1],
                    device_id={"grp": mate}, device_id_type=MESH).wait_recv()

    def q_copy(r, d):
        here = pl.ds(r * rows, rows)
        return pltpu.make_async_remote_copy(
            src_ref=square_ref.at[here], dst_ref=squares.at[d - 1, here],
            send_sem=q_send.at[r, d - 1], recv_sem=q_recv.at[r, d - 1],
            device_id={"tp": lax.rem(part + d, parts)}, device_id_type=MESH)

    def prepare(r):
        if fused:
            sum_chunk(r)
        for d in range(1, parts):
            y_copy(r, d).start()
        x_start(r, 0)
        for d in range(1, parts):
            q_copy(r, d).start()

    if fused:
        for copy in fills:
            copy.wait()

    def set_scale(r):
        here = pl.ds(r * rows, rows)
        mean_square = square_ref[here]
        for d in range(1, parts):
            q_copy(r, d).wait_recv()
            mean_square = mean_square + squares[d - 1, here]
        scale_ref[here] = lax.rsqrt(mean_square / (feature_share * parts) + epsilon)

    def wf_copy(j, at_core):
        at = wide.at[w_rows(1 - side, at_core), columns(j)]
        return pltpu.make_async_remote_copy(
            src_ref=at, dst_ref=at, send_sem=wf_send.at[j], recv_sem=wf_recv.at[j],
            device_id={"grp": mate}, device_id_type=MESH)

    def w_arrive(j):
        at = wide.at[w_rows(1 - side, core), columns(j)]
        pltpu.make_async_remote_copy(
            src_ref=at, dst_ref=at, send_sem=wx_send.at[j], recv_sem=wx_recv.at[j],
            device_id={"grp": across}, device_id_type=MESH).wait_recv()
        wf_copy(j, core).start()
        wf_copy(j, 1 - core).wait_recv()

    runs = []
    for r in range(chunks):
        before = min(columns_count, early + min(r - 1, 1)) if r else 0
        after = columns_count if r == chunks - 1 else min(columns_count, early + min(r, 1))
        if before:
            runs.append((r, 1, 0, before))
        if after > before:
            runs.append((0, r + 1, before, after))
    ends = [0]
    segments = [0] * chunks
    for r0, nr, j0, j1 in runs:
        ends.append(ends[-1] + nr * (j1 - j0))
        segments[r0 + nr - 1] = ends[-1]

    def place(s):
        r, j = s, s
        for (r0, nr, j0, _), begin in zip(runs, ends):
            inside = s >= begin
            r = jnp.where(inside, r0 + lax.rem(s - begin, nr), r)
            j = jnp.where(inside, j0 + (s - begin) // nr, j)
        return r, j

    def multiply(s):
        r, j = place(s)
        pl.when(r == 0)(functools.partial(w_arrive, j))
        products[lax.rem(s, slots)] = jnp.dot(
            xs[r], wide[:, columns(j)], preferred_element_type=jnp.float32)

    def chain(out, into, send, recv, s, blocks, to):
        return pltpu.make_async_remote_copy(
            src_ref=out.at[s, pl.ds(0, blocks)], dst_ref=into.at[s, pl.ds(0, blocks)],
            send_sem=send.at[s], recv_sem=recv.at[s],
            device_id={"grp": grp(to, side, core)}, device_id_type=MESH)

    def line(z, going_right, act):
        distance = ranks - 1 - z if going_right else z
        out, into, send, recv = ((right_out, right_in, rt_send, rt_recv) if going_right
                                 else (left_out, left_in, lt_send, lt_recv))
        return functools.partial(act, z, 1 if going_right else -1, distance,
                                 out, into, send, recv)

    def pass_line(z, sign, distance, out, into, send, recv, s):
        ends = ranks - 1 - distance
        slot = lax.rem(s, slots)
        if ends:
            chain(out, into, send, recv, s, distance + 1, z).wait_recv()
        for b in range(distance):
            block = z + sign * (b + 1)
            value = products[slot, pl.ds(block * rows, rows)]
            if ends:
                value = value + into[s, b + 1].astype(jnp.float32)
            out[s, b] = value.astype(jnp.bfloat16)
        if distance:
            chain(out, into, send, recv, s, distance, z + sign).start()

    def drain_line(z, sign, distance, out, into, send, recv, s):
        if distance:
            chain(out, into, send, recv, s, distance, z + sign).wait_send()

    def finish(z, s):
        r, j = place(s)
        slot = lax.rem(s, slots)
        here = pl.ds(pl.multiple_of(r * rows, rows), rows)
        total = products[slot, pl.ds(z * rows, rows)]
        if z:
            total = total + right_in[s, 0].astype(jnp.float32)
        if z < ranks - 1:
            total = total + left_in[s, 0].astype(jnp.float32)
        total = total * scale_ref[here, :][:, :1] + bias_row[:, columns(j)]
        total = total.astype(jnp.bfloat16)

        def to_query():
            query_ref[here, columns(j)] = total

        def to_keyval():
            keyval_ref[here, columns(j - q_steps)] = total

        pl.when(j < q_steps)(to_query)
        pl.when(j >= q_steps)(to_keyval)

    def step(i, carry):
        pl.when(i < steps)(functools.partial(multiply, i))
        for z in range(ranks):
            def at_rank(z=z):
                for going_right in (True, False):
                    lag = LAG * (z if going_right else ranks - 1 - z)
                    s = i - lag
                    pl.when(jnp.logical_and(s >= 0, s < steps))(
                        functools.partial(line(z, going_right, pass_line), s))
                s = i - LAG * max(z, ranks - 1 - z)
                pl.when(jnp.logical_and(s >= 0, s < steps))(functools.partial(finish, z, s))

            pl.when(rank == z)(at_rank)
        return carry

    def load_own():
        for copy in locals_:
            copy.wait()
        theirs = w_rows(side, 1 - core)
        for i, (src, dst) in enumerate(((wq_ref, wide.at[theirs, pl.ds(0, q_cols)]),
                                        (wk_ref, wide.at[theirs, pl.ds(q_cols, k_cols)]))):
            pltpu.make_async_remote_copy(
                src_ref=src, dst_ref=dst, send_sem=m_send.at[i], recv_sem=m_recv.at[i],
                device_id={"grp": mate}, device_id_type=MESH).wait_recv()

    def segment(r):
        if r == 0:
            load_own()
        x_wait(r)
        set_scale(r)
        lax.fori_loop(segments[r - 1] if r else 0,
                      segments[r] + (LAG * (ranks - 1) if r == chunks - 1 else 0), step, 0)

    events = []
    for r in range(chunks):
        events += [(r, prepare, r), (r + 1.5, relay, r), (r + 2.6, pass_on, r),
                   (r + (4.55 if r else 3.7), segment, r)]
        if fused and r > 1:
            events.append((r - 1.9, send_part, r))
    for _, event, r in sorted(events, key=lambda e: e[0]):
        event(r)

    if fused:
        for r in range(chunks):
            for d in range(1, parts):
                p_copy(r, d).wait_send()
    for copy in m_copies:
        copy.wait_send()
    for r in range(chunks):
        for d in range(parts):
            each_x(r, d, lambda r, d, i: x_copy(r, d, i).wait_send(), None)
        for d in range(1, parts):
            y_copy(r, d).wait_send()
            for source in range(ranks):
                f_copy(r, source, d).wait_send()
        for d in range(1, parts):
            q_copy(r, d).wait_send()

    def drain_w(j, carry):
        at = wide.at[mine, columns(j)]
        pltpu.make_async_remote_copy(
            src_ref=at, dst_ref=at, send_sem=wx_send.at[j], recv_sem=wx_recv.at[j],
            device_id={"grp": across}, device_id_type=MESH).wait_send()
        wf_copy(j, core).wait_send()
        return carry

    lax.fori_loop(0, columns_count, drain_w, 0)

    def drain_steps(s, carry):
        for z in range(ranks):
            def at_rank(z=z):
                for going_right in (True, False):
                    line(z, going_right, drain_line)(s)

            pl.when(rank == z)(at_rank)
        return carry

    lax.fori_loop(0, steps, drain_steps, 0)


def project(state, w_query, w_keyval, biases, group, parts, fused):
    if fused:
        count, feature_share = state[1].shape
    else:
        count, feature_share = state[0].shape
    depth, q_cols = w_query.shape
    k_cols = w_keyval.shape[1]
    total = q_cols + k_cols
    width = math.gcd(math.gcd(q_cols, k_cols), 512)
    ranks = group // (CORES * SIDES)
    share = CORES * SIDES * depth
    chunks = min(4, count // (16 * parts))
    rows = count // chunks
    columns_count = total // width
    early = min(EARLY, columns_count)
    steps = chunks * columns_count
    slots = LAG * (ranks - 1) + 1
    held = ranks // parts
    vmem = pl.BlockSpec(memory_space=pltpu.VMEM)
    hbm = pl.BlockSpec(memory_space=pl.ANY)
    dma = pltpu.SemaphoreType.DMA
    bf16 = jnp.bfloat16
    line = pltpu.VMEM((steps, ranks - 1, rows, width), bf16)
    outs = [jax.ShapeDtypeStruct((count, q_cols), bf16),
            jax.ShapeDtypeStruct((count, k_cols), bf16)]
    scratch = []
    if fused:
        outs.insert(0, jax.ShapeDtypeStruct((count, feature_share), bf16))
        scratch = [
            pltpu.VMEM((count, feature_share), bf16),
            pltpu.VMEM((count, feature_share), bf16),
            pltpu.VMEM((parts - 1, count, feature_share), bf16),
            pltpu.VMEM((count, feature_share), bf16),
            pltpu.VMEM((count, 128), jnp.float32),
            pltpu.VMEM((1, feature_share), jnp.float32),
            dma((2,)), dma((chunks, parts - 1)), dma((chunks, parts - 1)),
        ]
    scratch += [
        pltpu.VMEM((1, total), jnp.float32),
        pltpu.VMEM((parts - 1, count // parts, feature_share), bf16),
        pltpu.VMEM((chunks, ranks * rows, share), bf16),
        pltpu.VMEM((share, total), bf16),
        pltpu.VMEM((slots, ranks * rows, width), jnp.float32),
        line, line, line, line,
        pltpu.VMEM((parts - 1, count, 128), jnp.float32),
        pltpu.VMEM((count, 128), jnp.float32),
        dma((2,)), dma((2,)), dma((2,)),
        dma((columns_count,)), dma((columns_count,)),
        dma((columns_count,)), dma((columns_count,)),
        dma((chunks, parts - 1)), dma((chunks, parts - 1)),
        dma((chunks, parts, held)), dma((chunks, ranks)),
        dma((chunks, ranks, parts - 1)), dma((chunks, ranks, parts - 1)),
        dma((chunks, parts - 1)), dma((chunks, parts - 1)),
        dma((steps,)), dma((steps,)), dma((steps,)), dma((steps,)),
    ]
    return pl.pallas_call(
        functools.partial(kernel, ranks, parts, chunks, width, early, fused),
        out_shape=tuple(outs),
        in_specs=([hbm, hbm, vmem] if fused else [vmem, vmem]) + [hbm, hbm, vmem, vmem],
        out_specs=(vmem,) * len(outs),
        scratch_shapes=scratch,
        compiler_params=pltpu.CompilerParams(
            collective_id=0, has_side_effects=True, vmem_limit_bytes=62 * 1024 * 1024),
    )(*state, w_query, w_keyval, *biases)


def hand_over(cuts, *refs):
    count = len(cuts)
    sources, targets = refs[:count], refs[count:2 * count]
    buffers, taken, given = refs[2 * count:3 * count], refs[-2], refs[-1]

    def copies(i, c):
        rows = sources[i].shape[0] // cuts[i]
        here = pl.ds(c * rows, rows)
        return (pltpu.make_async_copy(sources[i].at[here], buffers[i].at[here], taken.at[i, c]),
                pltpu.make_async_copy(buffers[i].at[here], targets[i].at[here], given.at[i, c]))

    every = [copies(i, c) for i in range(count) for c in range(cuts[i])]
    for copy, _ in every:
        copy.start()
    for copy, onward in every:
        copy.wait()
        onward.start()
    for _, onward in every:
        onward.wait()


def place(*arrays):
    cuts = [4 if a.shape[0] * a.shape[1] > 2 ** 18 and a.shape[0] % 64 == 0 else 1 for a in arrays]
    anywhere = pl.BlockSpec(memory_space=pl.ANY)
    dma = pltpu.SemaphoreType.DMA
    return pl.pallas_call(
        functools.partial(hand_over, cuts),
        out_shape=tuple(jax.ShapeDtypeStruct(a.shape, a.dtype) for a in arrays),
        in_specs=[anywhere] * len(arrays),
        out_specs=(anywhere,) * len(arrays),
        scratch_shapes=[pltpu.VMEM(a.shape, a.dtype) for a in arrays] + [
            dma((len(arrays), max(cuts))), dma((len(arrays), max(cuts)))],
    )(*arrays)


def local(group, parts, sections, partials, residual, norm_gain, w_query, w_keyval,
          bias_query, bias_keyval):
    feature_share = residual.shape[2]
    biases = (bias_query, bias_keyval)
    if sections == 1:
        seqs, length = residual.shape[:2]
        count = seqs * length
        hidden, query, keyval = project(
            (partials.reshape(count, -1), residual.reshape(count, -1), norm_gain),
            w_query, w_keyval, biases, group, parts, True)
        hidden, query, keyval = place(hidden, query, keyval)
        hidden = hidden.reshape(residual.shape)
    else:
        offset = lax.axis_index("tp") * feature_share
        local_gain = lax.dynamic_slice_in_dim(
            norm_gain, offset, feature_share, 0).astype(jnp.float32)
        summed = lax.psum_scatter(
            partials[0], "tp", scatter_dimension=2, tiled=True).astype(jnp.float32)
        hidden = (residual.astype(jnp.float32) + summed).astype(jnp.bfloat16)
        widened = hidden.astype(jnp.float32)
        squares = jnp.sum(widened * widened, axis=-1)
        scaled = (widened * local_gain).astype(jnp.bfloat16)
        scaled = lax.all_gather(scaled, "section", axis=0, tiled=True)
        squares = lax.all_gather(squares, "section", axis=0, tiled=True)
        seqs, length = squares.shape
        count = seqs * length
        squares = jnp.broadcast_to(squares.reshape(-1, 1), (count, 128))
        query, keyval = project(
            (scaled.reshape(count, feature_share), squares), w_query, w_keyval, biases,
            group, parts, False)
    return (hidden, query.reshape(seqs, length, -1), keyval.reshape(seqs, length, -1))


def solution(mesh):
    placed = (
        P("tp", "section", "grp", None),
        P("section", "grp", "tp"),
        P(),
        P("grp", ("section", "tp")),
        P("grp", ("section", "tp")),
        P(("section", "tp")),
        P(("section", "tp")),
    )
    return jax.shard_map(
        functools.partial(local, mesh.shape["grp"], mesh.shape["tp"], mesh.shape["section"]),
        mesh=mesh,
        in_specs=placed,
        out_specs=(
            P("section", "grp", "tp"),
            P(None, "grp", ("section", "tp")),
            P(None, "grp", ("section", "tp")),
        ),
        check_vma=False,
    )
```

```python
import functools
import math

import jax
import jax.numpy as jnp
from jax import lax
from jax.experimental import pallas as pl
from jax.experimental.pallas import tpu as pltpu
from jax.sharding import PartitionSpec as P

epsilon = 1e-06
MESH = pl.DeviceIdType.MESH
CORES = 2
SIDES = 2
LAG = 3
EARLY = 3


def kernel(ranks, parts, chunks, width, early, fused, *refs):
    refs = list(refs)
    take = lambda n: [refs.pop(0) for _ in range(n)]
    if fused:
        partial_ref, residual_ref, gain_ref = take(3)
    else:
        given_rows, given_squares = take(2)
    wq_ref, wk_ref, bias_q_ref, bias_k_ref = take(4)
    if fused:
        hidden_ref, = take(1)
    query_ref, keyval_ref = take(2)
    if fused:
        own_part, own_residual, part_in, rows_ref, square_ref = take(5)
        gain_row, h_local, p_send, p_recv = take(4)
    else:
        rows_ref, square_ref = given_rows, given_squares
    (bias_row, others, xs, wide, products, right_out, right_in, left_out, left_in, squares, scale_ref,
     w_local, m_send, m_recv, wx_send, wx_recv, wf_send, wf_recv,
     y_send, y_recv, x_send, x_recv, f_send, f_recv, q_send, q_recv,
     rt_send, rt_recv, lt_send, lt_recv) = refs

    me = lax.axis_index("grp")
    part = lax.axis_index("tp")
    core = lax.rem(me, CORES)
    chip = me // CORES
    side = lax.rem(chip, SIDES)
    rank = chip // SIDES
    depth, q_cols = wq_ref.shape
    k_cols = wk_ref.shape[1]
    share = SIDES * CORES * depth
    q_steps = q_cols // width
    columns_count = (q_cols + k_cols) // width
    count, feature_share = rows_ref.shape
    rows = count // chunks
    piece = rows // parts
    held = ranks // parts
    steps = chunks * columns_count
    slots = products.shape[0]

    def grp(at_rank, at_side, at_core):
        return (at_rank * SIDES + at_side) * CORES + at_core

    mate = grp(rank, side, 1 - core)
    across = grp(rank, 1 - side, core)

    if fused:
        fills = [
            pltpu.make_async_copy(
                partial_ref.at[:, pl.ds(pl.multiple_of(part * feature_share, feature_share),
                                        feature_share)], own_part, h_local.at[0]),
            pltpu.make_async_copy(residual_ref, own_residual, h_local.at[1])]
        for copy in fills:
            copy.start()

    def w_rows(at_side, at_core):
        return pl.ds(pl.multiple_of((at_side * CORES + at_core) * depth, depth), depth)

    mine = w_rows(side, core)
    locals_ = [pltpu.make_async_copy(wq_ref, wide.at[mine, pl.ds(0, q_cols)], w_local.at[0]),
               pltpu.make_async_copy(wk_ref, wide.at[mine, pl.ds(q_cols, k_cols)], w_local.at[1])]
    for copy in locals_:
        copy.start()

    barrier = pltpu.get_barrier_semaphore()
    for peer in (mate, across):
        pl.semaphore_signal(barrier, inc=1, device_id={"grp": peer}, device_id_type=MESH)
    for k in range(1, ranks):
        pl.semaphore_signal(
            barrier, inc=1, device_id={"grp": grp(lax.rem(rank + k, ranks), side, core)},
            device_id_type=MESH)
    for d in range(1, parts):
        pl.semaphore_signal(
            barrier, inc=1, device_id={"tp": lax.rem(part + d, parts)}, device_id_type=MESH)
    pl.semaphore_wait(barrier, ranks + parts)

    def spread(src, start, length, dst, to):
        block = math.gcd(length, 1024)
        for b in range(length // block):
            value = src[pl.ds(start + b * block, block)].astype(jnp.float32)
            dst[:, pl.ds(to + b * block, block)] = value.reshape(1, block)

    def p_copy(r, d):
        to = lax.rem(part + d, parts)
        return pltpu.make_async_remote_copy(
            src_ref=partial_ref.at[pl.ds(r * rows, rows),
                                   pl.ds(pl.multiple_of(to * feature_share, feature_share),
                                         feature_share)],
            dst_ref=part_in.at[d - 1, pl.ds(r * rows, rows)],
            send_sem=p_send.at[r, d - 1], recv_sem=p_recv.at[r, d - 1],
            device_id={"tp": to}, device_id_type=MESH)

    def send_part(r):
        for d in range(1, parts):
            p_copy(r, d).start()

    if fused:
        for r in range(min(2, chunks)):
            send_part(r)
        spread(gain_ref, pl.multiple_of(part * feature_share, feature_share), feature_share,
               gain_row, 0)
    spread(bias_q_ref, 0, q_cols, bias_row, 0)
    spread(bias_k_ref, 0, k_cols, bias_row, q_cols)

    def columns(j):
        return pl.ds(pl.multiple_of(j * width, width), width)

    def wx_copy(src, j, to_column):
        return pltpu.make_async_remote_copy(
            src_ref=src.at[:, columns(j)], dst_ref=wide.at[mine, columns(to_column)],
            send_sem=wx_send.at[to_column], recv_sem=wx_recv.at[to_column],
            device_id={"grp": across}, device_id_type=MESH)

    def start_q(j, carry):
        wx_copy(wq_ref, j, j).start()
        return carry

    def start_k(j, carry):
        wx_copy(wk_ref, j, q_steps + j).start()
        return carry

    lax.fori_loop(0, q_steps, start_q, 0)
    lax.fori_loop(0, columns_count - q_steps, start_k, 0)
    m_copies = [pltpu.make_async_remote_copy(
        src_ref=src, dst_ref=dst, send_sem=m_send.at[i], recv_sem=m_recv.at[i],
        device_id={"grp": mate}, device_id_type=MESH)
        for i, (src, dst) in enumerate(((wq_ref, wide.at[mine, pl.ds(0, q_cols)]),
                                        (wk_ref, wide.at[mine, pl.ds(q_cols, k_cols)])))]
    for copy in m_copies:
        copy.start()

    def sum_chunk(r):
        for d in range(1, parts):
            p_copy(r, d).wait_recv()
        here = pl.ds(r * rows, rows)
        block = math.gcd(feature_share, 512)

        def body(c, total):
            at = pl.ds(pl.multiple_of(c * block, block), block)
            value = own_part[here, at].astype(jnp.float32)
            for d in range(1, parts):
                value = value + part_in[d - 1, here, at].astype(jnp.float32)
            value = (own_residual[here, at].astype(jnp.float32) + value).astype(jnp.bfloat16)
            hidden_ref[here, at] = value
            value = value.astype(jnp.float32)
            rows_ref[here, at] = (value * gain_row[:, at]).astype(jnp.bfloat16)
            value = value * value
            for b in range(block // 128):
                total = total + value[:, b * 128:(b + 1) * 128]
            return total

        total = lax.fori_loop(0, feature_share // block, body, jnp.zeros((rows, 128), jnp.float32))
        square_ref[here, :] = jnp.broadcast_to(
            jnp.sum(total, axis=1, keepdims=True), (rows, 128))

    def piece_at(base, index):
        return pl.ds(pl.multiple_of(base + index * piece, piece), piece)

    def y_copy(r, d):
        to = lax.rem(part + d, parts)
        return pltpu.make_async_remote_copy(
            src_ref=rows_ref.at[piece_at(r * rows, to)],
            dst_ref=others.at[d - 1, pl.ds(r * piece, piece)],
            send_sem=y_send.at[r, d - 1], recv_sem=y_recv.at[r, d - 1],
            device_id={"tp": to}, device_id_type=MESH)

    def x_ends(r, d, i):
        features = pl.ds(i * share, share)
        src = (others.at[d - 1, pl.ds(r * piece, piece), features] if d
               else rows_ref.at[piece_at(r * rows, part), features])
        return src, xs.at[r, piece_at(rank * rows, part)]

    def x_to(d, i):
        return lax.rem(part + parts - d, parts) * held + i

    def x_copy(r, d, i):
        src, dst = x_ends(r, d, i)
        return pltpu.make_async_remote_copy(
            src_ref=src, dst_ref=dst, send_sem=x_send.at[r, d, i], recv_sem=x_recv.at[r, rank],
            device_id={"grp": grp(x_to(d, i), side, core)}, device_id_type=MESH)

    def each_x(r, d, far, near):
        for i in range(held):
            here = x_to(d, i) == rank
            if near is not None:
                pl.when(here)(functools.partial(near, r, d, i))
            pl.when(jnp.logical_not(here))(functools.partial(far, r, d, i))

    def x_near(r, d, i):
        src, dst = x_ends(r, d, i)
        dst[...] = src[...]

    def x_start(r, d):
        each_x(r, d, lambda r, d, i: x_copy(r, d, i).start(), x_near)

    def relay(r):
        for d in range(1, parts):
            y_copy(r, d).wait_recv()
            x_start(r, d)

    def f_copy(r, source, d):
        at = xs.at[r, piece_at(source * rows, part)]
        return pltpu.make_async_remote_copy(
            src_ref=at, dst_ref=at,
            send_sem=f_send.at[r, source, d - 1], recv_sem=f_recv.at[r, source, d - 1],
            device_id={"tp": lax.rem(part + d, parts)}, device_id_type=MESH)

    def pass_on(r):
        for k in range(ranks):
            source = lax.rem(rank + k, ranks)
            if k:
                at = xs.at[r, piece_at(source * rows, part)]
                pltpu.make_async_remote_copy(
                    src_ref=at, dst_ref=at, send_sem=x_send.at[r, 0, 0],
                    recv_sem=x_recv.at[r, source],
                    device_id={"grp": mate}, device_id_type=MESH).wait_recv()
            for d in range(1, parts):
                f_copy(r, source, d).start()

    def x_wait(r):
        for source in range(ranks):
            for d in range(1, parts):
                at = xs.at[r, piece_at(source * rows, lax.rem(part + parts - d, parts))]
                pltpu.make_async_remote_copy(
                    src_ref=at, dst_ref=at,
                    send_sem=f_send.at[r, source, d - 1], recv_sem=f_recv.at[r, source, d - 1],
                    device_id={"grp": mate}, device_id_type=MESH).wait_recv()

    def q_copy(r, d):
        here = pl.ds(r * rows, rows)
        return pltpu.make_async_remote_copy(
            src_ref=square_ref.at[here], dst_ref=squares.at[d - 1, here],
            send_sem=q_send.at[r, d - 1], recv_sem=q_recv.at[r, d - 1],
            device_id={"tp": lax.rem(part + d, parts)}, device_id_type=MESH)

    def prepare(r):
        if fused:
            sum_chunk(r)
        for d in range(1, parts):
            y_copy(r, d).start()
        x_start(r, 0)
        for d in range(1, parts):
            q_copy(r, d).start()

    if fused:
        for copy in fills:
            copy.wait()

    def set_scale(r):
        here = pl.ds(r * rows, rows)
        mean_square = square_ref[here]
        for d in range(1, parts):
            q_copy(r, d).wait_recv()
            mean_square = mean_square + squares[d - 1, here]
        scale_ref[here] = lax.rsqrt(mean_square / (feature_share * parts) + epsilon)

    def wf_copy(j, at_core):
        at = wide.at[w_rows(1 - side, at_core), columns(j)]
        return pltpu.make_async_remote_copy(
            src_ref=at, dst_ref=at, send_sem=wf_send.at[j], recv_sem=wf_recv.at[j],
            device_id={"grp": mate}, device_id_type=MESH)

    def w_forward(j):
        at = wide.at[w_rows(1 - side, core), columns(j)]
        pltpu.make_async_remote_copy(
            src_ref=at, dst_ref=at, send_sem=wx_send.at[j], recv_sem=wx_recv.at[j],
            device_id={"grp": across}, device_id_type=MESH).wait_recv()
        wf_copy(j, core).start()

    def w_arrive(j):
        pl.when(j >= early)(functools.partial(w_forward, j))
        wf_copy(j, 1 - core).wait_recv()

    runs = []
    for r in range(chunks):
        before = min(columns_count, early + min(r - 1, 1)) if r else 0
        after = columns_count if r == chunks - 1 else min(columns_count, early + min(r, 1))
        if before:
            runs.append((r, 1, 0, before))
        if after > before:
            runs.append((0, r + 1, before, after))
    ends = [0]
    segments = [0] * chunks
    for r0, nr, j0, j1 in runs:
        ends.append(ends[-1] + nr * (j1 - j0))
        segments[r0 + nr - 1] = ends[-1]

    def place(s):
        r, j = s, s
        for (r0, nr, j0, _), begin in zip(runs, ends):
            inside = s >= begin
            r = jnp.where(inside, r0 + lax.rem(s - begin, nr), r)
            j = jnp.where(inside, j0 + (s - begin) // nr, j)
        return r, j

    def multiply(s):
        r, j = place(s)
        pl.when(r == 0)(functools.partial(w_arrive, j))
        products[lax.rem(s, slots)] = jnp.dot(
            xs[r], wide[:, columns(j)], preferred_element_type=jnp.float32)

    def chain(out, into, send, recv, s, distance, far, to):
        blocks = pl.ds(distance - 1, 1) if far else pl.ds(0, distance - 1)
        return pltpu.make_async_remote_copy(
            src_ref=out.at[s, blocks], dst_ref=into.at[s, blocks],
            send_sem=send.at[s, int(far)], recv_sem=recv.at[s, int(far)],
            device_id={"grp": grp(to, side, core)}, device_id_type=MESH)

    def line(z, going_right, act):
        distance = ranks - 1 - z if going_right else z
        out, into, send, recv = ((right_out, right_in, rt_send, rt_recv) if going_right
                                 else (left_out, left_in, lt_send, lt_recv))
        return functools.partial(act, z, 1 if going_right else -1, distance,
                                 out, into, send, recv)

    def pass_line(z, sign, distance, out, into, send, recv, s):
        ends = ranks - 1 - distance
        slot = lax.rem(s, slots)
        for far in (True, False):
            if ends and (far or distance):
                chain(out, into, send, recv, s, distance + 1, far, z).wait_recv()
            for b in range(max(distance - 1, 0), distance) if far else range(distance - 1):
                block = z + sign * (b + 1)
                value = products[slot, pl.ds(block * rows, rows)]
                if ends:
                    value = value + into[s, b + 1].astype(jnp.float32)
                out[s, b] = value.astype(jnp.bfloat16)
            if distance > (0 if far else 1):
                chain(out, into, send, recv, s, distance, far, z + sign).start()

    def drain_line(z, sign, distance, out, into, send, recv, s):
        for far in (True, False):
            if distance > (0 if far else 1):
                chain(out, into, send, recv, s, distance, far, z + sign).wait_send()

    def finish(z, s):
        r, j = place(s)
        slot = lax.rem(s, slots)
        here = pl.ds(pl.multiple_of(r * rows, rows), rows)
        total = products[slot, pl.ds(z * rows, rows)]
        if z:
            total = total + right_in[s, 0].astype(jnp.float32)
        if z < ranks - 1:
            total = total + left_in[s, 0].astype(jnp.float32)
        total = total * scale_ref[here, :][:, :1] + bias_row[:, columns(j)]
        total = total.astype(jnp.bfloat16)

        def to_query():
            query_ref[here, columns(j)] = total

        def to_keyval():
            keyval_ref[here, columns(j - q_steps)] = total

        pl.when(j < q_steps)(to_query)
        pl.when(j >= q_steps)(to_keyval)

    def step(i, carry):
        pl.when(i < steps)(functools.partial(multiply, i))
        for z in range(ranks):
            def at_rank(z=z):
                for going_right in (True, False):
                    lag = LAG * (z if going_right else ranks - 1 - z)
                    s = i - lag
                    pl.when(jnp.logical_and(s >= 0, s < steps))(
                        functools.partial(line(z, going_right, pass_line), s))
                s = i - LAG * max(z, ranks - 1 - z)
                pl.when(jnp.logical_and(s >= 0, s < steps))(functools.partial(finish, z, s))

            pl.when(rank == z)(at_rank)
        return carry

    def load_own():
        for copy in locals_:
            copy.wait()
        theirs = w_rows(side, 1 - core)
        for i, (src, dst) in enumerate(((wq_ref, wide.at[theirs, pl.ds(0, q_cols)]),
                                        (wk_ref, wide.at[theirs, pl.ds(q_cols, k_cols)]))):
            pltpu.make_async_remote_copy(
                src_ref=src, dst_ref=dst, send_sem=m_send.at[i], recv_sem=m_recv.at[i],
                device_id={"grp": mate}, device_id_type=MESH).wait_recv()

    def segment(r):
        if r == 0:
            load_own()
            for j in range(early):
                w_forward(j)
        x_wait(r)
        set_scale(r)
        lax.fori_loop(segments[r - 1] if r else 0,
                      segments[r] + (LAG * (ranks - 1) if r == chunks - 1 else 0), step, 0)

    events = []
    for r in range(chunks):
        events += [(r, prepare, r), (r + 1.5, relay, r), (r + 2.6, pass_on, r),
                   (r + (4.55 if r else 3.7), segment, r)]
        if fused and r > 1:
            events.append((r - 1.9, send_part, r))
    for _, event, r in sorted(events, key=lambda e: e[0]):
        event(r)

    if fused:
        for r in range(chunks):
            for d in range(1, parts):
                p_copy(r, d).wait_send()
    for copy in m_copies:
        copy.wait_send()
    for r in range(chunks):
        for d in range(parts):
            each_x(r, d, lambda r, d, i: x_copy(r, d, i).wait_send(), None)
        for d in range(1, parts):
            y_copy(r, d).wait_send()
            for source in range(ranks):
                f_copy(r, source, d).wait_send()
        for d in range(1, parts):
            q_copy(r, d).wait_send()

    def drain_w(j, carry):
        at = wide.at[mine, columns(j)]
        pltpu.make_async_remote_copy(
            src_ref=at, dst_ref=at, send_sem=wx_send.at[j], recv_sem=wx_recv.at[j],
            device_id={"grp": across}, device_id_type=MESH).wait_send()
        wf_copy(j, core).wait_send()
        return carry

    lax.fori_loop(0, columns_count, drain_w, 0)

    def drain_steps(s, carry):
        for z in range(ranks):
            def at_rank(z=z):
                for going_right in (True, False):
                    line(z, going_right, drain_line)(s)

            pl.when(rank == z)(at_rank)
        return carry

    lax.fori_loop(0, steps, drain_steps, 0)


def project(state, w_query, w_keyval, biases, group, parts, fused):
    if fused:
        count, feature_share = state[1].shape
    else:
        count, feature_share = state[0].shape
    depth, q_cols = w_query.shape
    k_cols = w_keyval.shape[1]
    total = q_cols + k_cols
    width = math.gcd(math.gcd(q_cols, k_cols), 512)
    ranks = group // (CORES * SIDES)
    share = CORES * SIDES * depth
    chunks = min(4, count // (16 * parts))
    rows = count // chunks
    columns_count = total // width
    early = min(EARLY, columns_count)
    steps = chunks * columns_count
    slots = LAG * (ranks - 1) + 1
    held = ranks // parts
    vmem = pl.BlockSpec(memory_space=pltpu.VMEM)
    hbm = pl.BlockSpec(memory_space=pl.ANY)
    dma = pltpu.SemaphoreType.DMA
    bf16 = jnp.bfloat16
    line = pltpu.VMEM((steps, ranks - 1, rows, width), bf16)
    outs = [jax.ShapeDtypeStruct((count, q_cols), bf16),
            jax.ShapeDtypeStruct((count, k_cols), bf16)]
    scratch = []
    if fused:
        outs.insert(0, jax.ShapeDtypeStruct((count, feature_share), bf16))
        scratch = [
            pltpu.VMEM((count, feature_share), bf16),
            pltpu.VMEM((count, feature_share), bf16),
            pltpu.VMEM((parts - 1, count, feature_share), bf16),
            pltpu.VMEM((count, feature_share), bf16),
            pltpu.VMEM((count, 128), jnp.float32),
            pltpu.VMEM((1, feature_share), jnp.float32),
            dma((2,)), dma((chunks, parts - 1)), dma((chunks, parts - 1)),
        ]
    scratch += [
        pltpu.VMEM((1, total), jnp.float32),
        pltpu.VMEM((parts - 1, count // parts, feature_share), bf16),
        pltpu.VMEM((chunks, ranks * rows, share), bf16),
        pltpu.VMEM((share, total), bf16),
        pltpu.VMEM((slots, ranks * rows, width), jnp.float32),
        line, line, line, line,
        pltpu.VMEM((parts - 1, count, 128), jnp.float32),
        pltpu.VMEM((count, 128), jnp.float32),
        dma((2,)), dma((2,)), dma((2,)),
        dma((columns_count,)), dma((columns_count,)),
        dma((columns_count,)), dma((columns_count,)),
        dma((chunks, parts - 1)), dma((chunks, parts - 1)),
        dma((chunks, parts, held)), dma((chunks, ranks)),
        dma((chunks, ranks, parts - 1)), dma((chunks, ranks, parts - 1)),
        dma((chunks, parts - 1)), dma((chunks, parts - 1)),
        dma((steps, 2)), dma((steps, 2)), dma((steps, 2)), dma((steps, 2)),
    ]
    return pl.pallas_call(
        functools.partial(kernel, ranks, parts, chunks, width, early, fused),
        out_shape=tuple(outs),
        in_specs=([hbm, hbm, vmem] if fused else [vmem, vmem]) + [hbm, hbm, vmem, vmem],
        out_specs=(vmem,) * len(outs),
        scratch_shapes=scratch,
        compiler_params=pltpu.CompilerParams(
            collective_id=0, has_side_effects=True, vmem_limit_bytes=62 * 1024 * 1024),
    )(*state, w_query, w_keyval, *biases)


def hand_over(cuts, *refs):
    count = len(cuts)
    sources, targets = refs[:count], refs[count:2 * count]
    buffers, taken, given = refs[2 * count:3 * count], refs[-2], refs[-1]

    def copies(i, c):
        rows = sources[i].shape[0] // cuts[i]
        here = pl.ds(c * rows, rows)
        return (pltpu.make_async_copy(sources[i].at[here], buffers[i].at[here], taken.at[i, c]),
                pltpu.make_async_copy(buffers[i].at[here], targets[i].at[here], given.at[i, c]))

    every = [copies(i, c) for i in range(count) for c in range(cuts[i])]
    for copy, _ in every:
        copy.start()
    for copy, onward in every:
        copy.wait()
        onward.start()
    for _, onward in every:
        onward.wait()


def place(*arrays):
    cuts = [4 if a.shape[0] * a.shape[1] > 2 ** 18 and a.shape[0] % 64 == 0 else 1 for a in arrays]
    anywhere = pl.BlockSpec(memory_space=pl.ANY)
    dma = pltpu.SemaphoreType.DMA
    return pl.pallas_call(
        functools.partial(hand_over, cuts),
        out_shape=tuple(jax.ShapeDtypeStruct(a.shape, a.dtype) for a in arrays),
        in_specs=[anywhere] * len(arrays),
        out_specs=(anywhere,) * len(arrays),
        scratch_shapes=[pltpu.VMEM(a.shape, a.dtype) for a in arrays] + [
            dma((len(arrays), max(cuts))), dma((len(arrays), max(cuts)))],
    )(*arrays)


def local(group, parts, sections, partials, residual, norm_gain, w_query, w_keyval,
          bias_query, bias_keyval):
    feature_share = residual.shape[2]
    biases = (bias_query, bias_keyval)
    if sections == 1:
        seqs, length = residual.shape[:2]
        count = seqs * length
        hidden, query, keyval = project(
            (partials.reshape(count, -1), residual.reshape(count, -1), norm_gain),
            w_query, w_keyval, biases, group, parts, True)
        hidden, query, keyval = place(hidden, query, keyval)
        hidden = hidden.reshape(residual.shape)
    else:
        offset = lax.axis_index("tp") * feature_share
        local_gain = lax.dynamic_slice_in_dim(
            norm_gain, offset, feature_share, 0).astype(jnp.float32)
        summed = lax.psum_scatter(
            partials[0], "tp", scatter_dimension=2, tiled=True).astype(jnp.float32)
        hidden = (residual.astype(jnp.float32) + summed).astype(jnp.bfloat16)
        widened = hidden.astype(jnp.float32)
        squares = jnp.sum(widened * widened, axis=-1)
        scaled = (widened * local_gain).astype(jnp.bfloat16)
        scaled = lax.all_gather(scaled, "section", axis=0, tiled=True)
        squares = lax.all_gather(squares, "section", axis=0, tiled=True)
        seqs, length = squares.shape
        count = seqs * length
        squares = jnp.broadcast_to(squares.reshape(-1, 1), (count, 128))
        query, keyval = project(
            (scaled.reshape(count, feature_share), squares), w_query, w_keyval, biases,
            group, parts, False)
    return (hidden, query.reshape(seqs, length, -1), keyval.reshape(seqs, length, -1))


def solution(mesh):
    placed = (
        P("tp", "section", "grp", None),
        P("section", "grp", "tp"),
        P(),
        P("grp", ("section", "tp")),
        P("grp", ("section", "tp")),
        P(("section", "tp")),
        P(("section", "tp")),
    )
    return jax.shard_map(
        functools.partial(local, mesh.shape["grp"], mesh.shape["tp"], mesh.shape["section"]),
        mesh=mesh,
        in_specs=placed,
        out_specs=(
            P("section", "grp", "tp"),
            P(None, "grp", ("section", "tp")),
            P(None, "grp", ("section", "tp")),
        ),
        check_vma=False,
    )
```
